128 devices in a mesh: tp: 4 (over z), cp: 4 (over y), fsdp: 8 (over x, core).
Axes of the slice: x: 4, y: 4, z: 4, core: 2. Of those that a mesh axis runs over, the one named last changes fastest.
Arguments:
- hidden: bfloat16 [8, 2048, 4608], P('fsdp', 'cp')
- cotangent: bfloat16 [8, 2048, 4608], P('fsdp', 'cp')
- positions: int32 [2048], P('cp')
- gain: bfloat16 [4608], P('fsdp')
- w_query: bfloat16 [4608, 32, 128], P('fsdp', 'tp')
- w_key: bfloat16 [4608, 16, 128], P('fsdp', 'tp')
- w_value: bfloat16 [4608, 16, 128], P('fsdp', 'tp')
- w_out: bfloat16 [32, 128, 4608], P('tp', None, 'fsdp')
Outputs:
- output 1: bfloat16 [8, 2048, 4608], P('fsdp', 'cp')
- output 2: bfloat16 [8, 2048, 4608], P('fsdp', 'cp')
- output 3: float32 [4608], P('fsdp')
- output 4: float32 [4608, 32, 128], P('fsdp', 'tp')
- output 5: float32 [4608, 16, 128], P('fsdp', 'tp')
- output 6: float32 [4608, 16, 128], P('fsdp', 'tp')
- output 7: float32 [32, 128, 4608], P('tp', None, 'fsdp')
All inputs are finite; a program needn't handle non-finite values.
Results may differ from the reference program's by a relative error of at most 0.0138296.
Values are sent between devices in bfloat16 or wider.
A program may use at most 1 GiB of HBM per device.

```python
import math
import jax
import jax.numpy as jnp
from jax import lax

BATCH_ROWS = 8
SEQ_LEN = 2048
MODEL_DIM = 4608
NUM_HEADS = 32
NUM_KV = 16
HEAD_DIM = 128
WINDOW_LEN = 4096

ROPE_BASE = 10000.0
NORM_EPS = 1e-5
NEG_BIG = -1e30
GROUP_SIZE = NUM_HEADS // NUM_KV
Q_BLOCK = math.gcd(SEQ_LEN, 512)
KEY_SPAN = min(Q_BLOCK + WINDOW_LEN, SEQ_LEN)


def setup_inputs(seed: int = 0) -> dict:
    key_list = jax.random.split(jax.random.key(seed), 9)
    act_shape = (BATCH_ROWS, SEQ_LEN, MODEL_DIM)
    hidden = jax.random.normal(key_list[0], act_shape, jnp.float32)
    cotangent = jax.random.normal(key_list[1], act_shape, jnp.float32)
    step_key, start_key = jax.random.split(key_list[2])
    pos_steps = jax.random.randint(step_key, (SEQ_LEN,), 1, 3)
    pos_start = jax.random.randint(start_key, (), 0, 64)
    positions = (pos_start + jnp.cumsum(pos_steps) - pos_steps[0]).astype(jnp.int32)
    gain = 1.0 + 0.5 * jax.random.normal(key_list[3], (MODEL_DIM,), jnp.float32)
    in_scale = MODEL_DIM ** -0.5
    out_scale = (NUM_HEADS * HEAD_DIM) ** -0.5
    w_query = jax.random.normal(key_list[4], (MODEL_DIM, NUM_HEADS, HEAD_DIM), jnp.float32) * in_scale
    w_key = jax.random.normal(key_list[5], (MODEL_DIM, NUM_KV, HEAD_DIM), jnp.float32) * in_scale
    w_value = jax.random.normal(key_list[6], (MODEL_DIM, NUM_KV, HEAD_DIM), jnp.float32) * in_scale
    w_out = jax.random.normal(key_list[7], (NUM_HEADS, HEAD_DIM, MODEL_DIM), jnp.float32) * out_scale
    return {"hidden": hidden.astype(jnp.bfloat16), "cotangent": cotangent.astype(jnp.bfloat16), "positions": positions, "gain": gain.astype(jnp.bfloat16), "w_query": w_query.astype(jnp.bfloat16), "w_key": w_key.astype(jnp.bfloat16), "w_value": w_value.astype(jnp.bfloat16), "w_out": w_out.astype(jnp.bfloat16)}


def to_bf16(vals_in):
    return vals_in + lax.stop_gradient(vals_in.astype(jnp.bfloat16).astype(jnp.float32) - vals_in)


def rope_tables(positions):
    inv_freq = ROPE_BASE ** (-jnp.arange(0, HEAD_DIM, 2).astype(jnp.float32) / HEAD_DIM)
    angles = positions.astype(jnp.float32)[:, None] * inv_freq[None, :]
    return jnp.cos(angles), jnp.sin(angles)


def rope_apply(head_vals, cosines, sines):
    half_dim = HEAD_DIM // 2
    first_half = head_vals[..., :half_dim]
    second_half = head_vals[..., half_dim:]
    cos_b = cosines[:, None, :]
    sin_b = sines[:, None, :]
    return jnp.concatenate([first_half * cos_b - second_half * sin_b, second_half * cos_b + first_half * sin_b], axis=-1)


def row_forward(x_row, param_set, cosines, sines):
    gain, w_query, w_key, w_value, w_out = param_set
    inv_rms = lax.rsqrt(jnp.mean(x_row * x_row, axis=-1, keepdims=True) + NORM_EPS)
    normed = to_bf16(x_row * inv_rms * gain)
    q_rot = to_bf16(rope_apply(jnp.einsum("sm,mhd->shd", normed, w_query), cosines, sines))
    k_rot = to_bf16(rope_apply(jnp.einsum("sm,mhd->shd", normed, w_key), cosines, sines))
    v_val = to_bf16(jnp.einsum("sm,mhd->shd", normed, w_value))
    q_grp = q_rot.reshape(SEQ_LEN, NUM_KV, GROUP_SIZE, HEAD_DIM)
    score_scale = HEAD_DIM ** -0.5

    def attend_block(blk_idx):
        q_start = blk_idx * Q_BLOCK
        k_start = jnp.clip(q_start + Q_BLOCK - KEY_SPAN, 0, SEQ_LEN - KEY_SPAN)
        q_blk = lax.dynamic_slice_in_dim(q_grp, q_start, Q_BLOCK, 0)
        k_blk = lax.dynamic_slice_in_dim(k_rot, k_start, KEY_SPAN, 0)
        v_blk = lax.dynamic_slice_in_dim(v_val, k_start, KEY_SPAN, 0)
        q_idx = q_start + jnp.arange(Q_BLOCK)
        k_idx = k_start + jnp.arange(KEY_SPAN)
        allowed = (k_idx[None, :] <= q_idx[:, None]) & (k_idx[None, :] > q_idx[:, None] - WINDOW_LEN)
        scores = jnp.einsum("qkgd,skd->kgqs", q_blk, k_blk) * score_scale
        scores = jnp.where(allowed, scores, NEG_BIG)
        prob_vals = to_bf16(jax.nn.softmax(scores, axis=-1))
        return to_bf16(jnp.einsum("kgqs,skd->qkgd", prob_vals, v_blk))

    attn_out = lax.map(jax.checkpoint(attend_block), jnp.arange(SEQ_LEN // Q_BLOCK))
    attn_out = attn_out.reshape(SEQ_LEN, NUM_HEADS, HEAD_DIM)
    return x_row + jnp.einsum("shd,hdm->sm", attn_out, w_out)


def reference(hidden, cotangent, positions, gain, w_query, w_key, w_value, w_out):
    cosines, sines = rope_tables(positions)
    params = tuple(weight.astype(jnp.float32) for weight in (gain, w_query, w_key, w_value, w_out))

    def row_step(grad_acc, row_pair):
        x_row, ct_row = row_pair
        out_row, pullback = jax.vjp(lambda x_in, param_set: row_forward(x_in, param_set, cosines, sines), x_row.astype(jnp.float32), params)
        dx_row, grad_parts = pullback(ct_row.astype(jnp.float32))
        grad_acc = tuple(grad_sum + grad_part for grad_sum, grad_part in zip(grad_acc, grad_parts))
        return grad_acc, (out_row.astype(jnp.bfloat16), dx_row.astype(jnp.bfloat16))

    zero_grads = tuple(jnp.zeros_like(weight) for weight in params)
    grad_tuple, row_outs = lax.scan(row_step, zero_grads, (hidden, cotangent))
    return (row_outs[0], row_outs[1], grad_tuple[0], grad_tuple[1], grad_tuple[2], grad_tuple[3], grad_tuple[4])
```

```python
import functools
import math

import jax
import jax.numpy as jnp
from jax import lax
from jax.experimental import pallas as pl
from jax.experimental.pallas import tpu as pltpu
from jax.sharding import PartitionSpec as P

WINDOW_LEN = 4096
ROPE_BASE = 10000.0
NORM_EPS = 1e-5
NEG_BIG = -1e30
LOG2E = math.log2(math.e)
BF16, F32 = jnp.bfloat16, jnp.float32
VMEM_LIMIT = 56 * 1024 * 1024


def dot(lhs, rhs, lhs_dim, rhs_dim):
    return lax.dot_general(lhs, rhs, (((lhs_dim,), (rhs_dim,)), ((), ())), preferred_element_type=F32)


def reduce_ring(up, down, part, gate=lambda far: far):
    far_up, far_down = up(part(2, 0)), down(part(2, 1))
    near_up, near_down = up(part(1, 1)), down(part(3, 0))
    far_up, far_down = gate((far_up, far_down))
    sum_up = up(part(1, 0) + far_up)
    sum_down = down(part(3, 1) + far_down)
    return part(0, 0) + sum_up + near_down, part(0, 1) + near_up + sum_down


def gather_ring(up, down, low, high):
    one_low, back_high = up(low), down(high)
    one_high, back_low = up(high), down(low)
    return {0: (low, high), 1: (one_low, one_high), 3: (back_low, back_high), 2: (up(one_low), down(back_high))}


def shift(axis, size, step):
    pairs = [(src, (src + step) % size) for src in range(size)]
    return lambda vals: lax.ppermute(vals, axis, pairs)


def swap_cores(vals):
    return lax.ppermute(vals, "fsdp", [(src, src ^ 1) for src in range(8)])


def rotate(vals, cosines, sines, sign):
    return vals * cosines + pltpu.roll(vals, vals.shape[1] // 2, 1) * (sines * sign)


def proj_kernel(rope_tiles, head_dim, x_ref, w_ref, cos_ref, sin_ref, o_ref):
    prod = jnp.dot(x_ref[...], w_ref[...], preferred_element_type=F32)

    def rotated():
        for head in range(prod.shape[1] // head_dim):
            cols = slice(head * head_dim, (head + 1) * head_dim)
            o_ref[:, cols] = rotate(prod[:, cols], cos_ref[...], sin_ref[...], 1.0).astype(BF16)

    if rope_tiles >= pl.num_programs(0):
        rotated()
    else:
        pl.when(pl.program_id(0) < rope_tiles)(rotated)

        @pl.when(pl.program_id(0) >= rope_tiles)
        def _():
            o_ref[...] = prod.astype(BF16)


def project(normed, weight, cosines, sines, rope_tiles):
    rows, depth = normed.shape
    cols, tile = weight.shape[1], 512
    head_dim = cosines.shape[1]
    whole = lambda shape: pl.BlockSpec(shape, lambda i: (0, 0))
    return pl.pallas_call(
        functools.partial(proj_kernel, rope_tiles, head_dim),
        grid=(cols // tile,),
        in_specs=[whole((rows, depth)), pl.BlockSpec((depth, tile), lambda i: (0, i)), whole((rows, head_dim)), whole((rows, head_dim))],
        out_specs=pl.BlockSpec((rows, tile), lambda i: (0, i)),
        out_shape=jax.ShapeDtypeStruct((rows, cols), BF16),
        compiler_params=pltpu.CompilerParams(vmem_limit_bytes=VMEM_LIMIT),
        cost_estimate=pl.CostEstimate(flops=2 * rows * depth * cols, bytes_accessed=2 * depth * (rows + cols), transcendentals=0),
        name="project",
    )(normed, weight, cosines, sines)


def block_mask(shape, key_dim, q_start, key_start):
    q_idx = q_start + lax.broadcasted_iota(jnp.int32, shape, 1 - key_dim)
    k_idx = key_start + lax.broadcasted_iota(jnp.int32, shape, key_dim)
    return (k_idx <= q_idx) & (k_idx > q_idx - WINDOW_LEN)


def needs_mask(block, length):
    return block == 0 or (block + 1) * length - 1 >= WINDOW_LEN


def attn_fwd_kernel(tile, cp_ref, q_ref, *refs):
    k_refs, v_refs = refs[0:4], refs[4:8]
    o_ref, lse_ref = refs[8:]
    length, head_dim = q_ref.shape
    scale = head_dim**-0.5 * LOG2E

    def one_tile(blocks, step, carry):
        start = pl.multiple_of(step * tile, tile)
        q_blk = q_ref[pl.ds(start, tile), :]
        scores = []
        for block in range(blocks):
            part = dot(k_refs[block][...], q_blk, 1, 1)
            if needs_mask(block, length):
                part = jnp.where(block_mask(part.shape, 0, start, -block * length), part, NEG_BIG)
            scores.append(part)
        top = functools.reduce(jnp.maximum, [jnp.max(part, axis=0, keepdims=True) for part in scores]) * scale
        powers = [jnp.exp2(part * scale - top) for part in scores]
        total = sum(jnp.sum(part, axis=0, keepdims=True) for part in powers)
        inverse = 1.0 / total
        out = sum(dot(v_refs[block][...], (powers[block] * inverse).astype(BF16), 0, 0) for block in range(blocks))
        o_ref[pl.ds(start, tile), :] = out.T.astype(BF16)
        lse_ref[0, :, pl.ds(start, tile)] = jnp.broadcast_to(top + jnp.log2(total), (8, tile))
        return carry

    for rank in range(4):

        @pl.when(cp_ref[0] == rank)
        def _():
            lax.fori_loop(0, length // tile, functools.partial(one_tile, rank + 1), 0)


def attn_forward(rank, q_rot, kv_blocks, head_dim):
    length, width = q_rot.shape
    heads = width // head_dim
    kv_heads = kv_blocks[0][0].shape[1] // head_dim
    group = heads // kv_heads
    tile = 256
    q_spec = pl.BlockSpec((length, head_dim), lambda h, cp: (0, h))
    kv_spec = pl.BlockSpec((length, head_dim), lambda h, cp: (0, h // group))
    return pl.pallas_call(
        functools.partial(attn_fwd_kernel, tile),
        grid_spec=pltpu.PrefetchScalarGridSpec(
            num_scalar_prefetch=1,
            grid=(heads,),
            in_specs=[q_spec] + [kv_spec] * 8,
            out_specs=[q_spec, pl.BlockSpec((1, 8, length), lambda h, cp: (h, 0, 0))],
        ),
        out_shape=[jax.ShapeDtypeStruct((length, width), BF16), jax.ShapeDtypeStruct((heads, 8, length), F32)],
        compiler_params=pltpu.CompilerParams(vmem_limit_bytes=VMEM_LIMIT),
        cost_estimate=pl.CostEstimate(flops=4 * 4 * length * length * width, bytes_accessed=20 * length * width, transcendentals=4 * length * length * heads),
        name="attn_forward",
    )(rank, q_rot, *(blk[0] for blk in kv_blocks), *(blk[1] for blk in kv_blocks))


def attn_bwd_kernel(tile, cp_ref, q_ref, do_ref, o_ref, lse_ref, cos_ref, sin_ref, *refs):
    k_refs, v_refs = refs[0:4], refs[4:8]
    dq_ref, dk_refs, dv_refs = refs[8], refs[9:13], refs[13:17]
    length, head_dim = q_ref.shape
    score_scale = head_dim**-0.5
    scale = score_scale * LOG2E

    @pl.when(pl.program_id(1) == 0)
    def _():
        for ref in (*dk_refs, *dv_refs):
            ref[...] = jnp.zeros_like(ref)

    def one_tile(blocks, step, carry):
        start = pl.multiple_of(step * tile, tile)
        rows = pl.ds(start, tile)
        q_blk, do_blk = q_ref[rows, :], do_ref[rows, :]
        row_dot = jnp.sum((do_blk.astype(F32) * o_ref[rows, :].astype(F32)).T, axis=0, keepdims=True)
        log_norm = lse_ref[0, 0:1, rows]
        d_query = jnp.zeros((tile, head_dim), F32)
        for block in range(blocks):
            k_blk, v_blk = k_refs[block][...], v_refs[block][...]
            probs = jnp.exp2(dot(k_blk, q_blk, 1, 1) * scale - log_norm)
            if needs_mask(block, length):
                probs = jnp.where(block_mask(probs.shape, 0, start, -block * length), probs, 0.0)
            d_scores = (probs * (dot(v_blk, do_blk, 1, 1) - row_dot) * score_scale).astype(BF16)
            dv_refs[block][...] += jnp.dot(probs.astype(BF16), do_blk, preferred_element_type=F32)
            dk_refs[block][...] += jnp.dot(d_scores, q_blk, preferred_element_type=F32)
            d_query += dot(d_scores, k_blk, 0, 0)
        dq_ref[rows, :] = rotate(d_query, cos_ref[rows, :], sin_ref[rows, :], -1.0).astype(BF16)
        return carry

    for rank in range(4):

        @pl.when(cp_ref[0] == rank)
        def _():
            lax.fori_loop(0, length // tile, functools.partial(one_tile, rank + 1), 0)


def attn_backward(rank, q_rot, d_attn, attn_out, log_norm, cosines, sines, kv_blocks):
    length, width = q_rot.shape
    head_dim = cosines.shape[1]
    heads, kv_heads = width // head_dim, kv_blocks[0][0].shape[1] // head_dim
    group = heads // kv_heads
    tile = 256
    q_spec = pl.BlockSpec((length, head_dim), lambda g, h, cp: (0, g * group + h))
    kv_spec = pl.BlockSpec((length, head_dim), lambda g, h, cp: (0, g))
    table = pl.BlockSpec((length, head_dim), lambda g, h, cp: (0, 0))
    kv_grad = jax.ShapeDtypeStruct(kv_blocks[0][0].shape, F32)
    outs = pl.pallas_call(
        functools.partial(attn_bwd_kernel, tile),
        grid_spec=pltpu.PrefetchScalarGridSpec(
            num_scalar_prefetch=1,
            grid=(kv_heads, group),
            in_specs=[q_spec, q_spec, q_spec, pl.BlockSpec((1, 8, length), lambda g, h, cp: (g * group + h, 0, 0)), table, table] + [kv_spec] * 8,
            out_specs=[q_spec] + [kv_spec] * 8,
        ),
        out_shape=[jax.ShapeDtypeStruct((length, width), BF16)] + [kv_grad] * 8,
        compiler_params=pltpu.CompilerParams(vmem_limit_bytes=VMEM_LIMIT),
        cost_estimate=pl.CostEstimate(flops=10 * 4 * length * length * width, bytes_accessed=30 * length * width, transcendentals=4 * length * length * heads),
        name="attn_backward",
    )(rank, q_rot, d_attn, attn_out, log_norm, cosines, sines, *(blk[0] for blk in kv_blocks), *(blk[1] for blk in kv_blocks))
    return outs[0], outs[1:5], outs[5:9]


def kv_grad_kernel(dk_ref, dv_ref, cos_ref, sin_ref, o_ref):
    head_dim, width = cos_ref.shape[1], dk_ref.shape[1]
    for head in range(width // head_dim):
        cols = slice(head * head_dim, (head + 1) * head_dim)
        o_ref[:, cols] = rotate(dk_ref[:, cols], cos_ref[...], sin_ref[...], -1.0).astype(BF16)
    o_ref[:, width:] = dv_ref[...].astype(BF16)


def kv_grad(d_keys, d_vals, cosines, sines):
    rows, width = d_keys.shape
    return pl.pallas_call(
        kv_grad_kernel,
        out_shape=jax.ShapeDtypeStruct((rows, 2 * width), BF16),
        compiler_params=pltpu.CompilerParams(vmem_limit_bytes=VMEM_LIMIT),
        cost_estimate=pl.CostEstimate(flops=4 * rows * width, bytes_accessed=12 * rows * width, transcendentals=0),
        name="kv_grad",
    )(d_keys, d_vals, cosines, sines)


def remote(src, dst, send_sem, recv_sem, axis, where):
    return pltpu.make_async_remote_copy(src_ref=src, dst_ref=dst, send_sem=send_sem, recv_sem=recv_sem, device_id={axis: where}, device_id_type=pl.DeviceIdType.MESH)


def finish_kernel(extra, *refs):
    low_ref, high_ref, cols_ref = refs[:3]
    refs = refs[3:]
    if extra:
        extra_ref, refs = refs[0], refs[1:]
    out_low, out_high, out_cols = refs[:3]
    refs = refs[3:]
    if extra:
        out_extra, refs = refs[0], refs[1:]
    land, sums, send, recv, local = refs[:5]
    cp, tp = lax.axis_index("cp"), lax.axis_index("tp")
    width = cols_ref.shape[1]
    y_up, y_down, y_far = lax.rem(cp + 1, 4), lax.rem(cp + 3, 4), lax.rem(cp + 2, 4)
    z_up, z_down = lax.rem(tp + 1, 4), lax.rem(tp + 3, 4)
    half = cols_ref.shape[0] // 2
    low_rows, high_rows = pl.ds(0, half), pl.ds(half, half)

    fsdp = lax.axis_index("fsdp")
    peers = [("cp", y_up), ("cp", y_down), ("tp", z_up), ("tp", z_down)]
    if extra == "gain":
        peers += [("cp", y_far), ("tp", lax.rem(tp + 2, 4))] + [("fsdp", lax.rem(fsdp + k, 8)) for k in range(1, 8)]
    barrier = pltpu.get_barrier_semaphore()
    for axis, where in peers:
        pl.semaphore_signal(barrier, inc=1, device_id={axis: where}, device_id_type=pl.DeviceIdType.MESH)
    pl.semaphore_wait(barrier, len(peers))

    def place(device, rows):
        return out_cols.at[rows, pl.ds(pl.multiple_of(device * width, width), width)]

    def start(index, src, dst, axis, where):
        copy = remote(src, dst, send.at[index], recv.at[index], axis, where)
        copy.start()
        return copy

    if extra == "gain":
        heard, told = refs[5:]
        over_y = [start(21 + k, extra_ref, heard.at[k - 1], "cp", lax.rem(cp + k, 4)) for k in range(1, 4)]
    far_up = start(0, low_ref.at[y_far], land.at[0], "cp", y_up)
    far_down = start(1, high_ref.at[y_far], land.at[1], "cp", y_down)
    z_one = start(6, cols_ref.at[low_rows], place(tp, low_rows), "tp", z_up)
    z_back = start(7, cols_ref.at[high_rows], place(tp, high_rows), "tp", z_down)
    z_one_more = start(8, cols_ref.at[high_rows], place(tp, high_rows), "tp", z_up)
    z_back_more = start(9, cols_ref.at[low_rows], place(tp, low_rows), "tp", z_down)
    near_up = start(2, high_ref.at[y_up], land.at[2], "cp", y_up)
    near_down = start(3, low_ref.at[y_down], land.at[3], "cp", y_down)
    mine = pltpu.make_async_copy(cols_ref, place(tp, pl.ds(0, 2 * half)), local.at[0])
    mine.start()

    far_up.wait()
    sums[0] = low_ref[y_up] + land[0]
    sum_up = start(4, sums.at[0], land.at[4], "cp", y_up)
    far_down.wait()
    sums[1] = high_ref[y_down] + land[1]
    sum_down = start(5, sums.at[1], land.at[5], "cp", y_down)

    if extra == "gain":
        for copy in over_y:
            copy.wait()
        told[...] = extra_ref[...] + heard[0] + heard[1] + heard[2]
        over_x = [start(24 + k, told, heard.at[k + 2], "fsdp", lax.rem(fsdp + k, 8)) for k in range(1, 8)]
    z_one.wait()
    z_two = start(10, place(z_down, low_rows), place(z_down, low_rows), "tp", z_up)
    z_back.wait()
    z_two_back = start(11, place(z_up, high_rows), place(z_up, high_rows), "tp", z_down)

    if extra == "gain":
        for copy in over_x:
            copy.wait()
        out_extra[tp] = told[...] + sum(heard[slot] for slot in range(3, 10))
        over_z = [start(31 + k, out_extra.at[tp], out_extra.at[tp], "tp", lax.rem(tp + k, 4)) for k in range(1, 4)]
    if extra == "rows":
        e_half = extra_ref.shape[0] // 2
        top, bottom = pl.ds(0, e_half), pl.ds(e_half, e_half)
        e_one = start(18, extra_ref, out_extra.at[cp], "cp", y_up)
        e_back = start(19, extra_ref, out_extra.at[cp], "cp", y_down)
        e_mine = pltpu.make_async_copy(extra_ref, out_extra.at[cp], local.at[1])
        e_mine.start()

    near_up.wait()
    near_down.wait()
    sum_up.wait()
    out_low[cp] = low_ref[cp] + land[4] + land[3]
    g_low = start(12, out_low.at[cp], out_low.at[cp], "cp", y_up)
    sum_down.wait()
    out_high[cp] = high_ref[cp] + land[2] + land[5]
    g_high = start(13, out_high.at[cp], out_high.at[cp], "cp", y_down)
    g_low_more = start(14, out_low.at[cp], out_low.at[cp], "cp", y_down)
    g_high_more = start(15, out_high.at[cp], out_high.at[cp], "cp", y_up)
    g_low.wait()
    g_low_two = start(16, out_low.at[y_down], out_low.at[y_down], "cp", y_up)
    g_high.wait()
    g_high_two = start(17, out_high.at[y_up], out_high.at[y_up], "cp", y_down)
    pending = [z_one_more, z_back_more, z_two, z_two_back, g_low_more, g_high_more, g_low_two, g_high_two]
    if extra == "gain":
        pending += over_z
    if extra == "rows":
        e_one.wait()
        pending.append(start(20, out_extra.at[y_down, top], out_extra.at[y_down, top], "cp", y_up))
        e_back.wait()
        pending.append(start(21, out_extra.at[y_up, bottom], out_extra.at[y_up, bottom], "cp", y_down))
        e_mine.wait()
    for copy in pending:
        copy.wait()
    mine.wait()


def finish(collective_id, low, high, cols, kind, extra):
    ins = [low, high, cols, extra]
    outs = [jax.ShapeDtypeStruct(low.shape, F32), jax.ShapeDtypeStruct(high.shape, F32), jax.ShapeDtypeStruct((cols.shape[0], 4 * cols.shape[1]), BF16)]
    outs.append(jax.ShapeDtypeStruct((4, *extra.shape), F32))
    vmem = pl.BlockSpec(memory_space=pltpu.VMEM)
    return pl.pallas_call(
        functools.partial(finish_kernel, kind),
        in_specs=[vmem] * len(ins),
        out_specs=[vmem] * len(outs),
        out_shape=outs,
        scratch_shapes=[
            pltpu.VMEM((6, *low.shape[1:]), F32),
            pltpu.VMEM((2, *low.shape[1:]), F32),
            pltpu.SemaphoreType.DMA((35 if kind == "gain" else 22,)),
            pltpu.SemaphoreType.DMA((35 if kind == "gain" else 22,)),
            pltpu.SemaphoreType.DMA((2,)),
        ]
        + ([pltpu.VMEM((10, *extra.shape), F32), pltpu.VMEM(extra.shape, F32)] if kind == "gain" else []),
        compiler_params=pltpu.CompilerParams(collective_id=collective_id, has_side_effects=True, vmem_limit_bytes=VMEM_LIMIT),
        cost_estimate=pl.CostEstimate(flops=40_000_000_000, bytes_accessed=8 * low.size, transcendentals=0),
        name=f"finish_{collective_id}",
    )(*ins)


def solution(mesh):
    act_spec = P("fsdp", "cp", None)
    proj_spec = P("fsdp", "tp", None)
    wout_spec = P("tp", None, "fsdp")

    def device_step(hidden, cotangent, positions, gain, w_query, w_key, w_value, w_out):
        x_in, cot = hidden[0], cotangent[0]
        length, width = x_in.shape
        shard, q_heads, head_dim = w_query.shape
        kv_heads = w_key.shape[1]
        q_width, kv_width = q_heads * head_dim, kv_heads * head_dim
        quarter, cols = shard // 4, width // 4
        tp, cp, fsdp = lax.axis_index("tp"), lax.axis_index("cp"), lax.axis_index("fsdp")
        x_pos, core = fsdp // 2, fsdp % 2
        tp_arr, cp_arr = jnp.reshape(tp, (1,)).astype(jnp.int32), jnp.reshape(cp, (1,)).astype(jnp.int32)
        z_up, z_down = shift("tp", 4, 1), shift("tp", 4, -1)
        y_up, y_down = shift("cp", 4, 1), shift("cp", 4, -1)
        x_up, x_down = shift("fsdp", 8, 2), shift("fsdp", 8, -2)

        def gather_weight(mat):
            mine = lax.dynamic_slice_in_dim(mat, cp * quarter, quarter, 0)
            return lax.all_gather(mine, ("fsdp", "cp"), axis=0, tiled=True)

        w_kv = gather_weight(jnp.concatenate([w_key.reshape(shard, kv_width), w_value.reshape(shard, kv_width)], axis=1))
        w_o = gather_weight(w_out.reshape(q_width, shard).T)

        wq_mine = w_query.reshape(shard, q_width)
        wq_ring = gather_ring(x_up, x_down, wq_mine[: shard // 2], wq_mine[shard // 2 :])
        wq_ring = jnp.stack([part for o in range(4) for part in wq_ring[o]]).reshape(4, shard, q_width)
        wq_other = swap_cores(wq_ring)
        w_q = jnp.zeros((4, 2, shard, q_width), BF16)
        for o in range(4):
            for chunks, side in ((wq_ring, core), (wq_other, 1 - core)):
                w_q = lax.dynamic_update_slice(w_q, chunks[o][None, None], ((x_pos - o) % 4, side, 0, 0))
        w_q = w_q.reshape(width, q_width)

        gains = jnp.stack([gain] + [shift("fsdp", 8, -k)(gain) for k in range(1, 8)])
        gain_full = lax.dynamic_slice_in_dim(jnp.concatenate([gains, gains]), 8 - fsdp, 8, 0).reshape(width).astype(F32)

        inv_freq = ROPE_BASE ** (-jnp.arange(0, head_dim, 2).astype(F32) / head_dim)
        angles = positions.astype(F32)[:, None] * inv_freq[None, :]
        cosines = jnp.concatenate([jnp.cos(angles)] * 2, axis=1)
        sines = jnp.concatenate([-jnp.sin(angles), jnp.sin(angles)], axis=1)

        x_f = x_in.astype(F32)
        inv_rms = lax.rsqrt(jnp.mean(x_f * x_f, axis=-1, keepdims=True) + NORM_EPS)
        normed = (x_f * inv_rms * gain_full).astype(BF16)

        kv_rot = project(normed, w_kv, cosines, sines, kv_width // 512)
        k_rot, v_loc = kv_rot[:, :kv_width], kv_rot[:, kv_width:]
        k_rot, v_loc, later, cot_later, x_later = lax.optimization_barrier((k_rot, v_loc, normed, cot, x_in))
        ring = gather_ring(y_up, y_down, k_rot, v_loc)
        kv_blocks = [ring[o] for o in range(4)]

        features = later.T.reshape(4, 2, shard, length)
        kept = lax.dynamic_index_in_dim(features, core, 1, keepdims=False)
        given = lax.dynamic_index_in_dim(features, 1 - core, 1, keepdims=False)
        cot_t = cot_later.T
        x_cols = lax.dynamic_slice_in_dim(x_later, tp * cols, cols, 1)
        cot_cols = lax.dynamic_slice_in_dim(cot_later, tp * cols, cols, 1)
        features = jnp.concatenate([kept, swap_cores(given)], axis=2)
        q_rot = project(normed, w_q, cosines, sines, q_width // 512)
        q_rot, features, cot_t, x_cols, cot_cols = lax.optimization_barrier((q_rot, features, cot_t, x_cols, cot_cols))
        x_cols, cot_cols = x_cols.astype(F32), cot_cols.astype(F32)
        d_attn = dot(cot, w_o, 1, 0).astype(BF16)
        attn_out, log_norm = attn_forward(cp_arr, q_rot, kv_blocks, head_dim)

        half = length // 2
        chunk_of = lambda mat, o: lax.dynamic_slice_in_dim(mat, ((tp + o) % 4) * cols, cols, 0)
        mixed = reduce_ring(z_up, z_down, lambda o, h: dot(attn_out[h * half : (h + 1) * half], chunk_of(w_o, o), 1, 1))
        out_cols = (x_cols + jnp.concatenate(mixed, axis=0)).astype(BF16)

        grad_wo = lax.psum_scatter(dot(cot_t, attn_out, 1, 0), ("fsdp", "cp"), scatter_dimension=0, tiled=True)

        dq_lin, dk_parts, dv_parts = attn_backward(cp_arr, q_rot, d_attn, attn_out, log_norm, cosines, sines, kv_blocks)

        def over_x(d_lin, gate):
            both = jnp.concatenate([d_lin, swap_cores(d_lin)], axis=0)
            wide = both.shape[1] // 2
            part = lambda o, h: dot(lax.dynamic_index_in_dim(features, (x_pos + o) % 4, 0, keepdims=False), both[:, h * wide : (h + 1) * wide], 1, 0)
            return [half.reshape(4, quarter, wide) for half in reduce_ring(x_up, x_down, part, gate)]

        gq_low, gq_high = over_x(dq_lin, lambda far: far)
        gq_low, gq_high, block_out, grad_wo = finish(0, gq_low, gq_high, out_cols, "rows", grad_wo)
        after_q = lambda far: lax.optimization_barrier((*far, gq_low))[:2]
        d_keys, d_vals = reduce_ring(y_up, y_down, lambda o, h: (dk_parts if h == 0 else dv_parts)[(4 - o) % 4])
        dkv_lin = kv_grad(d_keys, d_vals, cosines, sines)
        d_normed = reduce_ring(z_up, z_down, lambda o, h: dot(dq_lin[h * half : (h + 1) * half], chunk_of(w_q, o), 1, 1) + dot(dkv_lin[h * half : (h + 1) * half], chunk_of(w_kv, o), 1, 1), after_q)
        gk, gv = over_x(dkv_lin, after_q)

        grad_query = jnp.concatenate([gq_low.reshape(shard, -1), gq_high.reshape(shard, -1)], axis=1).reshape(shard, q_heads, head_dim)
        grad_wout = grad_wo.reshape(shard, q_width).T.reshape(q_heads, head_dim, shard)

        d_normed = jnp.concatenate(d_normed, axis=0)
        gain_cols = lax.dynamic_slice_in_dim(gain_full, tp * cols, cols, 0)
        x_hat = x_cols * inv_rms
        grad_gain = jnp.sum(d_normed * x_hat, axis=0)
        scaled = d_normed * gain_cols
        row_dot = jnp.sum(scaled * x_hat, axis=-1)
        row_dot = row_dot + sum(shift("tp", 4, k)(row_dot) for k in range(1, 4))
        grad_cols = (cot_cols + inv_rms * (scaled - x_hat * (row_dot / width)[:, None])).astype(BF16)
        grad_gain = jnp.pad(grad_gain, (0, 2048 - cols)).reshape(16, 128)
        gk, gv, grad_hidden, gain_all = finish(1, gk, gv, grad_cols, "gain", grad_gain)
        grad_key, grad_value = gk.reshape(shard, kv_heads, head_dim), gv.reshape(shard, kv_heads, head_dim)
        gain_all = gain_all.reshape(4, 2048)[:, :cols].reshape(width)
        grad_gain = lax.dynamic_slice_in_dim(gain_all, fsdp * shard, shard, 0)
        return block_out[None], grad_hidden[None], grad_gain, grad_query, grad_key, grad_value, grad_wout

    return jax.shard_map(device_step, mesh=mesh, in_specs=(act_spec, act_spec, P("cp"), P("fsdp"), proj_spec, proj_spec, proj_spec, wout_spec), out_specs=(act_spec, act_spec, P("fsdp"), proj_spec, proj_spec, proj_spec, wout_spec), check_vma=False)
```

```python
import functools
import math

import jax
import jax.numpy as jnp
from jax import lax
from jax.experimental import pallas as pl
from jax.experimental.pallas import tpu as pltpu
from jax.sharding import PartitionSpec as P

WINDOW_LEN = 4096
ROPE_BASE = 10000.0
NORM_EPS = 1e-5
NEG_BIG = -1e30
LOG2E = math.log2(math.e)
BF16, F32 = jnp.bfloat16, jnp.float32
VMEM_LIMIT = 56 * 1024 * 1024
VMEM_ALL = 67_043_328


def dot(lhs, rhs, lhs_dim, rhs_dim):
    return lax.dot_general(lhs, rhs, (((lhs_dim,), (rhs_dim,)), ((), ())), preferred_element_type=F32)


def gather_ring(up, down, low, high, gate):
    one_low, back_high = up(low), down(high)
    one_high, back_low = up(high), down(low)
    one_low, back_high = gate((one_low, back_high))
    return {0: (low, high), 1: (one_low, one_high), 3: (back_low, back_high), 2: (up(one_low), down(back_high))}


def shift(axis, size, step):
    pairs = [(src, (src + step) % size) for src in range(size)]
    return lambda vals: lax.ppermute(vals, axis, pairs)


def swap_cores(vals):
    return lax.ppermute(vals, "fsdp", [(src, src ^ 1) for src in range(8)])


def rotate(vals, cosines, sines, sign):
    return vals * cosines + pltpu.roll(vals, vals.shape[1] // 2, 1) * (sines * sign)


def proj_kernel(rope_tiles, head_dim, x_ref, w_ref, cos_ref, sin_ref, o_ref):
    prod = jnp.dot(x_ref[...], w_ref[...], preferred_element_type=F32)

    def rotated():
        for head in range(prod.shape[1] // head_dim):
            cols = slice(head * head_dim, (head + 1) * head_dim)
            o_ref[:, cols] = rotate(prod[:, cols], cos_ref[...], sin_ref[...], 1.0).astype(BF16)

    if rope_tiles >= pl.num_programs(0):
        rotated()
    else:
        pl.when(pl.program_id(0) < rope_tiles)(rotated)

        @pl.when(pl.program_id(0) >= rope_tiles)
        def _():
            o_ref[...] = prod.astype(BF16)


def project(normed, weight, cosines, sines, rope_tiles):
    rows, depth = normed.shape
    cols, tile = weight.shape[1], 512
    head_dim = cosines.shape[1]
    whole = lambda shape: pl.BlockSpec(shape, lambda i: (0, 0))
    return pl.pallas_call(
        functools.partial(proj_kernel, rope_tiles, head_dim),
        grid=(cols // tile,),
        in_specs=[whole((rows, depth)), pl.BlockSpec((depth, tile), lambda i: (0, i)), whole((rows, head_dim)), whole((rows, head_dim))],
        out_specs=pl.BlockSpec((rows, tile), lambda i: (0, i)),
        out_shape=jax.ShapeDtypeStruct((rows, cols), BF16),
        compiler_params=pltpu.CompilerParams(vmem_limit_bytes=VMEM_LIMIT),
        cost_estimate=pl.CostEstimate(flops=2 * rows * depth * cols, bytes_accessed=2 * depth * (rows + cols), transcendentals=0),
        name="project",
    )(normed, weight, cosines, sines)


def block_mask(shape, key_dim, q_start, key_start):
    q_idx = q_start + lax.broadcasted_iota(jnp.int32, shape, 1 - key_dim)
    k_idx = key_start + lax.broadcasted_iota(jnp.int32, shape, key_dim)
    return (k_idx <= q_idx) & (k_idx > q_idx - WINDOW_LEN)


def needs_mask(block, length):
    return block == 0 or (block + 1) * length - 1 >= WINDOW_LEN


def attn_fwd_kernel(tile, cp_ref, q_ref, *refs):
    k_refs, v_refs = refs[0:4], refs[4:8]
    o_ref, lse_ref = refs[8:]
    length, head_dim = q_ref.shape
    scale = head_dim**-0.5 * LOG2E

    def one_tile(blocks, step, carry):
        start = pl.multiple_of(step * tile, tile)
        q_blk = q_ref[pl.ds(start, tile), :]
        scores = []
        for block in range(blocks):
            part = dot(k_refs[block][...], q_blk, 1, 1)
            if needs_mask(block, length):
                part = jnp.where(block_mask(part.shape, 0, start, -block * length), part, NEG_BIG)
            scores.append(part)
        top = functools.reduce(jnp.maximum, [jnp.max(part, axis=0, keepdims=True) for part in scores]) * scale
        powers = [jnp.exp2(part * scale - top) for part in scores]
        total = sum(jnp.sum(part, axis=0, keepdims=True) for part in powers)
        inverse = 1.0 / total
        out = sum(dot(v_refs[block][...], (powers[block] * inverse).astype(BF16), 0, 0) for block in range(blocks))
        o_ref[pl.ds(start, tile), :] = out.T.astype(BF16)
        lse_ref[0, :, pl.ds(start, tile)] = jnp.broadcast_to(top + jnp.log2(total), (8, tile))
        return carry

    for rank in range(4):

        @pl.when(cp_ref[0] == rank)
        def _():
            lax.fori_loop(0, length // tile, functools.partial(one_tile, rank + 1), 0)


def attn_forward(rank, q_rot, kv_all, head_dim):
    length, width = q_rot.shape
    heads = width // head_dim
    kv_heads = kv_all.shape[2] // 2 // head_dim
    group = heads // kv_heads
    tile = 256
    q_spec = pl.BlockSpec((length, head_dim), lambda h, cp: (0, h))
    kv_spec = lambda o, first: pl.BlockSpec((None, length, head_dim), lambda h, cp: (lax.rem(cp[0] + 4 - o, 4), 0, first + h // group))
    return pl.pallas_call(
        functools.partial(attn_fwd_kernel, tile),
        grid_spec=pltpu.PrefetchScalarGridSpec(
            num_scalar_prefetch=1,
            grid=(heads,),
            in_specs=[q_spec] + [kv_spec(o, first) for first in (0, kv_heads) for o in range(4)],
            out_specs=[q_spec, pl.BlockSpec((1, 8, length), lambda h, cp: (h, 0, 0))],
        ),
        out_shape=[jax.ShapeDtypeStruct((length, width), BF16), jax.ShapeDtypeStruct((heads, 8, length), F32)],
        compiler_params=pltpu.CompilerParams(vmem_limit_bytes=VMEM_LIMIT),
        cost_estimate=pl.CostEstimate(flops=16 * length * length * width, bytes_accessed=20 * length * width, transcendentals=4 * length * length * heads),
        name="attn_forward",
    )(rank, q_rot, *[kv_all] * 8)


def attn_bwd_kernel(tile, cp_ref, q_ref, do_ref, o_ref, lse_ref, cos_ref, sin_ref, *refs):
    k_refs, v_refs = refs[0:4], refs[4:8]
    dq_ref, dk_refs, dv_refs = refs[8], refs[9:13], refs[13:17]
    length, head_dim = q_ref.shape
    score_scale = head_dim**-0.5
    scale = score_scale * LOG2E

    @pl.when(pl.program_id(1) == 0)
    def _():
        for ref in (*dk_refs, *dv_refs):
            ref[...] = jnp.zeros_like(ref)

    def one_tile(blocks, step, carry):
        start = pl.multiple_of(step * tile, tile)
        rows = pl.ds(start, tile)
        q_blk, do_blk = q_ref[rows, :], do_ref[rows, :]
        row_dot = jnp.sum((do_blk.astype(F32) * o_ref[rows, :].astype(F32)).T, axis=0, keepdims=True)
        log_norm = lse_ref[0, 0:1, rows]
        d_query = jnp.zeros((tile, head_dim), F32)
        for block in range(blocks):
            k_blk, v_blk = k_refs[block][...], v_refs[block][...]
            probs = jnp.exp2(dot(k_blk, q_blk, 1, 1) * scale - log_norm)
            if needs_mask(block, length):
                probs = jnp.where(block_mask(probs.shape, 0, start, -block * length), probs, 0.0)
            d_scores = (probs * (dot(v_blk, do_blk, 1, 1) - row_dot) * score_scale).astype(BF16)
            dv_refs[block][...] += jnp.dot(probs.astype(BF16), do_blk, preferred_element_type=F32)
            dk_refs[block][...] += jnp.dot(d_scores, q_blk, preferred_element_type=F32)
            d_query += dot(d_scores, k_blk, 0, 0)
        dq_ref[rows, :] = rotate(d_query, cos_ref[rows, :], sin_ref[rows, :], -1.0).astype(BF16)
        return carry

    for rank in range(4):

        @pl.when(cp_ref[0] == rank)
        def _():
            lax.fori_loop(0, length // tile, functools.partial(one_tile, rank + 1), 0)


def attn_backward(rank, q_rot, d_attn, attn_out, log_norm, cosines, sines, kv_all):
    length, width = q_rot.shape
    head_dim = cosines.shape[1]
    heads, kv_heads = width // head_dim, kv_all.shape[2] // 2 // head_dim
    group = heads // kv_heads
    tile = 256
    q_spec = pl.BlockSpec((length, head_dim), lambda g, h, cp: (0, g * group + h))
    kv_spec = pl.BlockSpec((length, head_dim), lambda g, h, cp: (0, g))
    table = pl.BlockSpec((length, head_dim), lambda g, h, cp: (0, 0))
    kv_in = lambda o, first: pl.BlockSpec((None, length, head_dim), lambda g, h, cp: (lax.rem(cp[0] + 4 - o, 4), 0, first + g))
    kv_grad = jax.ShapeDtypeStruct((length, kv_heads * head_dim), F32)
    outs = pl.pallas_call(
        functools.partial(attn_bwd_kernel, tile),
        grid_spec=pltpu.PrefetchScalarGridSpec(
            num_scalar_prefetch=1,
            grid=(kv_heads, group),
            in_specs=[q_spec, q_spec, q_spec, pl.BlockSpec((1, 8, length), lambda g, h, cp: (g * group + h, 0, 0)), table, table] + [kv_in(o, first) for first in (0, kv_heads) for o in range(4)],
            out_specs=[q_spec] + [kv_spec] * 8,
        ),
        out_shape=[jax.ShapeDtypeStruct((length, width), BF16)] + [kv_grad] * 8,
        compiler_params=pltpu.CompilerParams(vmem_limit_bytes=VMEM_LIMIT),
        cost_estimate=pl.CostEstimate(flops=40 * length * length * width, bytes_accessed=30 * length * width, transcendentals=4 * length * length * heads),
        name="attn_backward",
    )(rank, q_rot, d_attn, attn_out, log_norm, cosines, sines, *[kv_all] * 8)
    return outs[0], outs[1:5], outs[5:9]


def kv_grad_kernel(dk_ref, dv_ref, cos_ref, sin_ref, o_ref):
    head_dim, width = cos_ref.shape[1], dk_ref.shape[1]
    for head in range(width // head_dim):
        cols = slice(head * head_dim, (head + 1) * head_dim)
        o_ref[:, cols] = rotate(dk_ref[:, cols], cos_ref[...], sin_ref[...], -1.0).astype(BF16)
    o_ref[:, width:] = dv_ref[...].astype(BF16)


def kv_grad(d_keys, d_vals, cosines, sines):
    rows, width = d_keys.shape
    return pl.pallas_call(
        kv_grad_kernel,
        out_shape=jax.ShapeDtypeStruct((rows, 2 * width), BF16),
        compiler_params=pltpu.CompilerParams(vmem_limit_bytes=VMEM_LIMIT),
        name="kv_grad",
    )(d_keys, d_vals, cosines, sines)


MESH = pl.DeviceIdType.MESH


class Exchange:
    def __init__(self, collective_id):
        self.collective_id = collective_id
        self.entries, self.ins, self.in_specs, self.outs, self.out_specs, self.scratch = [], [], [], [], [], []
        self.sends = self.locals = 0

    def add(self, stages, axis, ins, outs, scratch, sends, locals_, space, out_space=pltpu.VMEM):
        self.entries.append((stages, axis, len(ins), len(outs), len(scratch), self.sends, self.locals))
        self.ins += ins
        spaces = space if isinstance(space, list) else [space] * len(ins)
        self.in_specs += [pl.BlockSpec(memory_space=kind) for kind in spaces]
        self.outs += outs
        self.out_specs += [pl.BlockSpec(memory_space=out_space)] * len(outs)
        self.scratch += scratch
        self.sends += sends
        self.locals += locals_

    def kernel(self, *refs):
        ins, refs = refs[: len(self.ins)], refs[len(self.ins) :]
        outs, refs = refs[: len(self.outs)], refs[len(self.outs) :]
        scratch, (send, recv, local) = refs[:-3], refs[-3:]
        where = {name: lax.axis_index(name) for name in ("tp", "cp", "fsdp")}
        steps = {"tp": (4, (1, 3)), "cp": (4, (1, 3)), "fsdp": (8, (2, 6))}
        wide = any(axis == "all" for _, axis, *_ in self.entries)
        steps_of = lambda axis: range(1, steps[axis][0]) if wide else steps[axis][1]
        axes = sorted({axis for _, axis, *_ in self.entries if axis not in ("all", "none")} | ({"tp", "cp", "fsdp"} if wide else set()))
        peers = [(axis, lax.rem(where[axis] + step, steps[axis][0])) for axis in axes for step in steps_of(axis)]
        barrier = pltpu.get_barrier_semaphore()
        for axis, peer in peers:
            pl.semaphore_signal(barrier, inc=1, device_id={axis: peer}, device_id_type=MESH)
        pl.semaphore_wait(barrier, len(peers))

        running = []
        for stages, axis, n_in, n_out, n_scratch, first_send, first_local in self.entries:

            def start(index, src, dst, axis, step, first_send=first_send):
                peer = lax.rem(where[axis] + step, steps[axis][0])
                sems = first_send + index
                copy = pltpu.make_async_remote_copy(src_ref=src, dst_ref=dst, send_sem=send.at[sems], recv_sem=recv.at[sems], device_id={axis: peer}, device_id_type=MESH)
                copy.start()
                return copy

            def load(index, src, dst, first_local=first_local):
                copy = pltpu.make_async_copy(src, dst, local.at[first_local + index])
                copy.start()
                return copy

            ring, place = start, where
            if axis not in ("all", "none"):
                size, (up, down) = steps[axis]
                ring = (functools.partial(lambda start, axis, step, i, s, d: start(i, s, d, axis, step), start, axis, up), functools.partial(lambda start, axis, step, i, s, d: start(i, s, d, axis, step), start, axis, down))
                place = where[axis] if size == 4 else where[axis] // 2
            running.append(stages(ins[:n_in], outs[:n_out], scratch[:n_scratch], ring, load, place))
            ins, outs, scratch = ins[n_in:], outs[n_out:], scratch[n_scratch:]
        left = []
        while running:
            turns = [(stage, next(stage, stage)) for stage in running]
            left += [copy for _, copies in turns if isinstance(copies, list) for copy in copies]
            running = [stage for stage, copies in turns if copies is not stage]
        for copy in left:
            copy.wait()

    def run(self):
        return pl.pallas_call(
            self.kernel,
            in_specs=self.in_specs,
            out_specs=self.out_specs,
            out_shape=self.outs,
            scratch_shapes=self.scratch + [pltpu.SemaphoreType.DMA((self.sends,)), pltpu.SemaphoreType.DMA((self.sends,)), pltpu.SemaphoreType.DMA((max(self.locals, 1),))],
            compiler_params=pltpu.CompilerParams(collective_id=self.collective_id, has_side_effects=True, vmem_limit_bytes=VMEM_ALL),
            cost_estimate=pl.CostEstimate(flops=40_000_000_000, bytes_accessed=40_000_000, transcendentals=0),
            name=f"exchange_{self.collective_id}",
        )(*self.ins)

    def ring_sum(self, axis, part):
        parts = [part(o, h) for o in range(4) for h in range(2)]
        half = jax.ShapeDtypeStruct(parts[0].shape, F32)
        self.add(given_ring_stages, axis, parts, [half] * 2, [pltpu.VMEM((8, *half.shape), F32), pltpu.VMEM((6, *half.shape), F32)], 6, 10, pl.ANY, pl.ANY)

    def weight_ring(self, features, d_lin):
        rows, cols = features.shape[1], d_lin.shape[1] // 2
        half = jax.ShapeDtypeStruct((rows, cols), F32)
        scratch = [pltpu.VMEM((8, rows, cols), F32), pltpu.VMEM((6, rows, cols), F32), pltpu.VMEM(features.shape, BF16), pltpu.VMEM(d_lin.shape, BF16)]
        self.add(weight_ring_stages, "fsdp", [features, d_lin], [half, half], scratch, 6, 10, pl.ANY, pl.ANY)

    def out_ring(self, attn_out, w_o, x_cols):
        rows, width = attn_out.shape
        cols = x_cols.shape[1]
        scratch = [pltpu.VMEM((8, rows // 2, cols), F32), pltpu.VMEM((6, rows // 2, cols), F32), pltpu.VMEM((2, cols, width), BF16)]
        out = jax.ShapeDtypeStruct(x_cols.shape, BF16)
        self.add(out_ring_stages, "tp", [attn_out, x_cols, w_o], [out], scratch, 6, 4, [pltpu.VMEM, pltpu.VMEM, pl.ANY])

    def normed_ring(self, dq_lin, dkv_lin, w_kv, wq_ring, wq_other):
        rows, width = dq_lin.shape[0] // 2, dq_lin.shape[1]
        cols = w_kv.shape[0] // 4
        half = jax.ShapeDtypeStruct((rows, cols), F32)
        scratch = [pltpu.VMEM((8, rows, cols), F32), pltpu.VMEM((6, rows, cols), F32), pltpu.VMEM((cols, width), BF16), pltpu.VMEM((cols, width), BF16)]
        self.add(normed_ring_stages, "tp", [dq_lin, dkv_lin, w_kv, wq_ring, wq_other], [half, half], scratch, 6, 10, [pltpu.VMEM] * 2 + [pl.ANY] * 3, pl.ANY)

    def project(self, normed, cosines, sines, wq_ring, wq_other):
        rows, depth = normed.shape
        cols = wq_ring.shape[2]
        scratch = [pltpu.VMEM((rows, depth), BF16), pltpu.VMEM((depth, cols), BF16)]
        self.add(project_stages, "none", [normed, cosines, sines, wq_ring, wq_other], [jax.ShapeDtypeStruct((rows, cols), BF16)], scratch, 0, 9, [pl.ANY, pltpu.VMEM, pltpu.VMEM, pl.ANY, pl.ANY])

    def all_sum(self, axis, low, high):
        outs = [jax.ShapeDtypeStruct(low.shape, F32)] * 2
        self.add(all_sum_stages, axis, [low, high], outs, [pltpu.VMEM((6, *low.shape[1:]), F32), pltpu.VMEM((2, *low.shape[1:]), F32)], 12, 0, pltpu.VMEM)

    def gather(self, axis, block, by_columns, late=0, pause=1):
        shape = (block.shape[0], 4 * block.shape[1]) if by_columns else (4, *block.shape)
        self.add(functools.partial(gather_stages, by_columns, late, pause), axis, [block], [jax.ShapeDtypeStruct(shape, block.dtype)], [], 6, 1, pltpu.VMEM)

    def small_sum(self, vals):
        out = jax.ShapeDtypeStruct((4, *vals.shape), F32)
        self.add(small_sum_stages, "all", [vals], [out], [pltpu.VMEM((10, *vals.shape), F32), pltpu.VMEM(vals.shape, F32)], 13, 0, pltpu.VMEM)


def add_rows(dst, *terms):
    step = math.gcd(dst.shape[0], 64)

    def body(index, carry):
        rows = pl.ds(pl.multiple_of(index * step, step), step)
        dst[rows, :] = sum(term[rows, :] for term in terms)
        return carry

    lax.fori_loop(0, dst.shape[0] // step, body, 0)


def reduce_steps(term, into, land, ring, compute):
    ways = list(zip(range(2), ring, (1, 3)))
    far, near, last = [], [], []
    for h, send, _ in ways:
        compute(2, h)
        far.append(send(h, term(2, h), land.at[h]))
    yield
    for h, send, o in ways:
        compute(o, 1 - h)
        near.append(send(2 + h, term(o, 1 - h), land.at[2 + h]))
        compute(o, h)
        yield
    for h, send, o in ways:
        far[h].wait()
        add_rows(into(o, h), term(o, h), land.at[h])
        last.append(send(4 + h, into(o, h), land.at[4 + h]))
    yield
    for h in range(2):
        compute(0, h)
    yield
    for copy in near:
        copy.wait()
    yield
    for h in range(2):
        last[h].wait()
        add_rows(into(0, h), term(0, h), land.at[4 + h], land.at[3 - h])


def gather_steps(source, at, ring, place, base, pause):
    up, down = ring
    ways = list(zip(range(2), (up, down), (down, up), (3, 1)))
    first, more = [], []
    for h, send, _, _ in ways:
        first.append(send(base + h, source(h), at(place, h)))
    for h, _, send, _ in ways:
        more.append(send(base + 2 + h, source(h), at(place, h)))
    for _ in range(pause):
        yield
    for h, send, _, step in ways:
        from_next = at(lax.rem(place + step, 4), h)
        first[h].wait()
        more.append(send(base + 4 + h, from_next, from_next))
    yield more


def store_halves(parts, outs, load, base):
    yield [load(base + h, parts.at[h], outs[h]) for h in range(2)]


def given_ring_stages(ins, outs, scratch, ring, load, place):
    parts, land = scratch
    loads = {slot: load(slot, ins[slot], parts.at[slot]) for slot in (4, 5, 3, 2, 6, 7, 0, 1)}
    term = lambda o, h: parts.at[2 * o + h]
    yield from reduce_steps(term, term, land, ring, lambda o, h: loads[2 * o + h].wait())
    yield from store_halves(parts, outs, load, 8)


def weight_ring_stages(ins, outs, scratch, ring, load, place):
    parts, land, features, d_lin = scratch
    loads = [load(0, ins[0], features), load(1, ins[1], d_lin)]
    cols = parts.shape[2]
    yield
    for copy in loads:
        copy.wait()

    def compute(o, h):
        parts[2 * o + h] = jnp.dot(features[lax.rem(place + o, 4)], d_lin[:, h * cols : (h + 1) * cols], preferred_element_type=F32)

    term = lambda o, h: parts.at[2 * o + h]
    yield from reduce_steps(term, term, land, ring, compute)
    yield from store_halves(parts, outs, load, 8)


def out_ring_stages(ins, outs, scratch, ring, load, place):
    (attn_out, x_cols, w_o), (out,), (parts, land, weights) = ins, outs, scratch
    rows, cols = parts.shape[1], parts.shape[2]
    order = [2, 1, 3, 0]
    fetch = lambda turn: load(turn, w_o.at[pl.ds(pl.multiple_of(lax.rem(place + order[turn], 4) * cols, cols), cols)], weights.at[turn % 2])
    pending = {0: fetch(0), 1: fetch(1)}
    yield

    def compute(o, h):
        turn = order.index(o)
        if turn in pending:
            pending.pop(turn).wait()
        parts[2 * o + h] = dot(attn_out[h * rows : (h + 1) * rows, :], weights[turn % 2], 1, 1)
        used[turn] = used.get(turn, 0) + 1
        if used[turn] == 2 and turn + 2 < 4:
            pending[turn + 2] = fetch(turn + 2)

    used = {}
    term = lambda o, h: parts.at[2 * o + h]
    yield from reduce_steps(term, term, land, ring, compute)
    for h in range(2):
        span = pl.ds(h * rows, rows)
        out[span, :] = (x_cols[span, :].astype(F32) + parts[h]).astype(BF16)


def normed_ring_stages(ins, outs, scratch, ring, load, place):
    (dq, dkv, w_kv, wq_ring, wq_other), (parts, land, kv_weights, q_weights) = ins, scratch
    rows, cols = parts.shape[1], parts.shape[2]
    shard = cols // 2
    fsdp = lax.axis_index("fsdp")
    x_pos, core = fsdp // 2, lax.rem(fsdp, 2)
    loaded = [None]

    def fetch(o):
        chunk = lax.rem(place + o, 4)
        piece = lax.rem(x_pos + 4 - chunk, 4)
        copies = [
            load(0, w_kv.at[pl.ds(pl.multiple_of(chunk * cols, cols), cols)], kv_weights),
            load(1, wq_ring.at[piece], q_weights.at[pl.ds(pl.multiple_of(core * shard, shard), shard)]),
            load(2, wq_other.at[piece], q_weights.at[pl.ds(pl.multiple_of((1 - core) * shard, shard), shard)]),
        ]
        loaded[0] = (o, copies)

    fetch(2)
    yield
    following = {2: 1, 1: 3, 3: 0}
    used = {}

    def compute(o, h):
        if loaded[0][1] is not None:
            for copy in loaded[0][1]:
                copy.wait()
            loaded[0] = (o, None)
        span = slice(h * rows, (h + 1) * rows)
        parts[2 * o + h] = dot(dq[span, :], q_weights[...], 1, 1) + dot(dkv[span, :], kv_weights[...], 1, 1)
        used[o] = used.get(o, 0) + 1
        if used[o] == 2 and o in following:
            fetch(following[o])

    term = lambda o, h: parts.at[2 * o + h]
    yield from reduce_steps(term, term, land, ring, compute)
    yield from store_halves(parts, outs, load, 8)


def project_stages(ins, outs, scratch, ring, load, place):
    (normed, cosines, sines, wq_ring, wq_other), (out,), (x_buf, w_buf) = ins, outs, scratch
    shard, head_dim = wq_ring.shape[1], cosines.shape[1]
    x_pos, core = place["fsdp"] // 2, lax.rem(place["fsdp"], 2)
    loads = [load(0, normed, x_buf)]
    for o in range(4):
        for side, pieces in enumerate((wq_ring, wq_other)):
            owner = lax.rem(x_pos + 4 - o, 4) * 2 + (core if side == 0 else 1 - core)
            loads.append(load(1 + 2 * o + side, pieces.at[o], w_buf.at[pl.ds(pl.multiple_of(owner * shard, shard), shard)]))
    yield
    for copy in loads:
        copy.wait()
    tile = 256

    def body(step, carry):
        span = pl.ds(pl.multiple_of(step * tile, tile), tile)
        prod = jnp.dot(x_buf[...], w_buf[:, span], preferred_element_type=F32)
        heads = [rotate(prod[:, h * head_dim : (h + 1) * head_dim], cosines[...], sines[...], 1.0) for h in range(tile // head_dim)]
        out[:, span] = jnp.concatenate(heads, axis=1).astype(BF16)
        return carry

    lax.fori_loop(0, w_buf.shape[1] // tile, body, 0)


def all_sum_stages(ins, outs, scratch, ring, load, place):
    land, sums = scratch
    term = lambda o, h: ins[h].at[lax.rem(place + o, 4)]
    into = lambda o, h: sums.at[h] if o else outs[h].at[place]
    yield from reduce_steps(term, into, land, ring, lambda o, h: None)
    at = lambda device, h: outs[h].at[device]
    yield from gather_steps(lambda h: at(place, h), at, ring, place, 6, 1)


def gather_stages(by_columns, late, pause, ins, outs, scratch, ring, load, place):
    (block,), (out,) = ins, outs
    rows, width = block.shape
    span = lambda h: pl.ds(h * (rows // 2), rows // 2)

    def at(device, rows):
        return out.at[rows, pl.ds(pl.multiple_of(device * width, width), width)] if by_columns else out.at[device, rows]

    for _ in range(late):
        yield
    mine = load(0, block, at(place, pl.ds(0, rows)))
    yield from gather_steps(lambda h: block.at[span(h)], lambda device, h: at(device, span(h)), ring, place, 0, pause)
    yield [mine]


def small_sum_stages(ins, outs, scratch, start, load, place):
    (vals,), (out,), (heard, told) = ins, outs, scratch
    over_y = [start(k - 1, vals, heard.at[k - 1], "cp", k) for k in range(1, 4)]
    yield
    for copy in over_y:
        copy.wait()
    told[...] = vals[...] + heard[0] + heard[1] + heard[2]
    over_x = [start(k + 2, told, heard.at[k + 2], "fsdp", k) for k in range(1, 8)]
    yield
    for copy in over_x:
        copy.wait()
    mine = place["tp"]
    out[mine] = told[...] + sum(heard[slot] for slot in range(3, 10))
    yield [start(k + 9, out.at[mine], out.at[mine], "tp", k) for k in range(1, 4)]


def solution(mesh):
    act_spec = P("fsdp", "cp", None)
    proj_spec = P("fsdp", "tp", None)
    wout_spec = P("tp", None, "fsdp")

    def device_step(hidden, cotangent, positions, gain, w_query, w_key, w_value, w_out):
        x_in, cot = hidden[0], cotangent[0]
        length, width = x_in.shape
        shard, q_heads, head_dim = w_query.shape
        kv_heads = w_key.shape[1]
        q_width, kv_width = q_heads * head_dim, kv_heads * head_dim
        quarter, cols = shard // 4, width // 4
        tp, cp, fsdp = lax.axis_index("tp"), lax.axis_index("cp"), lax.axis_index("fsdp")
        x_pos, core = fsdp // 2, fsdp % 2
        own_cols = lambda vals: lax.dynamic_slice_in_dim(vals, tp * cols, cols, -1)
        mat = lambda weight: weight.reshape(weight.shape[0], -1)
        tp_arr, cp_arr = jnp.reshape(tp, (1,)).astype(jnp.int32), jnp.reshape(cp, (1,)).astype(jnp.int32)
        x_up, x_down = shift("fsdp", 8, 2), shift("fsdp", 8, -2)

        def gather_weight(mat):
            mine = lax.dynamic_slice_in_dim(mat, cp * quarter, quarter)
            return lax.all_gather(mine, ("fsdp", "cp"), tiled=True)

        gains = jnp.stack([gain] + [shift("fsdp", 8, -2 * k)(gain) for k in range(1, 4)])
        others = swap_cores(gains)
        gains = jnp.stack([jnp.where(core == 0, gains, others), jnp.where(core == 0, others, gains)], axis=1)
        gain_full = lax.dynamic_slice_in_dim(jnp.concatenate([gains, gains]), 4 - x_pos, 4).reshape(width).astype(F32)

        w_kv = gather_weight(jnp.concatenate([mat(w_key), mat(w_value)], axis=1))
        w_o = lax.all_gather(w_out.reshape(q_width, shard).T, "fsdp", tiled=True)

        wq_mine = mat(w_query)
        wq_mine, gain_full = lax.optimization_barrier((wq_mine, gain_full))
        inv_freq = ROPE_BASE ** (-jnp.arange(0, head_dim, 2).astype(F32) / head_dim)
        angles = positions.astype(F32)[:, None] * inv_freq[None, :]
        cosines = jnp.concatenate([jnp.cos(angles)] * 2, axis=1)
        sines = jnp.concatenate([-jnp.sin(angles), jnp.sin(angles)], axis=1)

        x_f = x_in.astype(F32)
        inv_rms = lax.rsqrt(jnp.mean(x_f * x_f, axis=-1, keepdims=True) + NORM_EPS)
        normed = (x_f * inv_rms * gain_full).astype(BF16)

        features = normed.T.reshape(4, 2, shard, length)
        kept, given = (lax.dynamic_index_in_dim(features, side, 1, keepdims=False) for side in (core, 1 - core))
        cot_t = cot.T
        x_cols = own_cols(x_in)
        cot_cols = own_cols(cot)
        local = lambda arrays: lax.optimization_barrier((*arrays, normed, kept, given, cot_t, x_cols, cot_cols))
        wq_ring = gather_ring(x_up, x_down, wq_mine[: shard // 2], wq_mine[shard // 2 :], lambda landed: local(landed)[:2])
        wq_ring = jnp.stack([part for o in range(4) for part in wq_ring[o]]).reshape(4, shard, q_width)
        wq_other = swap_cores(wq_ring)
        w_kv, normed, kept, given, cot_t, x_cols, cot_cols = local((w_kv,))

        kv_rot = project(normed, w_kv, cosines, sines, kv_width // 512)
        features = jnp.concatenate([kept, swap_cores(given)], axis=2)
        front = Exchange(3)
        front.gather("cp", kv_rot, False)
        front.project(normed, cosines, sines, wq_ring, wq_other)
        kv_all, q_rot = front.run()
        d_attn = dot(cot, w_o, 1, 0).astype(BF16)
        attn_out, log_norm = attn_forward(cp_arr, q_rot, kv_all, head_dim)
        grad_wo = lax.psum_scatter(dot(cot_t, attn_out, 1, 0), ("fsdp", "cp"), tiled=True)

        dq_lin, dk_parts, dv_parts = attn_backward(cp_arr, q_rot, d_attn, attn_out, log_norm, cosines, sines, kv_all)

        both_cores = lambda d_lin: jnp.concatenate([d_lin, swap_cores(d_lin)])
        by_cp = lambda part: part.reshape(4, quarter, part.shape[1])
        first = Exchange(0)
        first.ring_sum("cp", lambda o, h: (dk_parts if h == 0 else dv_parts)[(4 - o) % 4])
        first.weight_ring(features, both_cores(dq_lin))
        first.out_ring(attn_out, w_o, x_cols)
        d_keys, d_vals, gq_low, gq_high, out_cols = first.run()

        dkv_lin = kv_grad(d_keys, d_vals, cosines, sines)

        second = Exchange(1)
        second.all_sum("cp", by_cp(gq_low), by_cp(gq_high))
        second.weight_ring(features, both_cores(dkv_lin))
        second.normed_ring(dq_lin, dkv_lin, w_kv, wq_ring, wq_other)
        second.gather("cp", grad_wo, False, 6, 2)
        gq_low, gq_high, gk, gv, dn_low, dn_high, grad_wo = second.run()

        grad_query = jnp.concatenate([gq_low.reshape(shard, -1), gq_high.reshape(shard, -1)], axis=1).reshape(shard, q_heads, head_dim)

        x_cols, cot_cols = x_cols.astype(F32), cot_cols.astype(F32)
        d_normed = jnp.concatenate([dn_low, dn_high])
        gain_cols = own_cols(gain_full)
        x_hat = x_cols * inv_rms
        grad_gain = jnp.sum(d_normed * x_hat, axis=0)
        scaled = d_normed * gain_cols
        row_dot = jnp.sum(scaled * x_hat, axis=-1)
        row_dot = row_dot + sum(shift("tp", 4, k)(row_dot) for k in range(1, 4))
        grad_cols = (cot_cols + inv_rms * (scaled - x_hat * (row_dot / width)[:, None])).astype(BF16)
        grad_gain = jnp.pad(grad_gain, (0, 2048 - cols)).reshape(16, 128)

        third = Exchange(2)
        third.small_sum(grad_gain)
        third.all_sum("cp", by_cp(gk), by_cp(gv))
        third.gather("tp", grad_cols, True, 0, 4)
        third.gather("tp", out_cols, True, 0, 8)
        gain_all, gk, gv, grad_hidden, block_out = third.run()
        grad_wout = grad_wo.reshape(shard, q_width).T.reshape(q_heads, head_dim, shard)
        grad_key, grad_value = gk.reshape(shard, kv_heads, head_dim), gv.reshape(shard, kv_heads, head_dim)
        gain_all = gain_all.reshape(4, 2048)[:, :cols].reshape(width)
        grad_gain = lax.dynamic_slice_in_dim(gain_all, fsdp * shard, shard, 0)
        return block_out[None], grad_hidden[None], grad_gain, grad_query, grad_key, grad_value, grad_wout

    return jax.shard_map(device_step, mesh=mesh, in_specs=(act_spec, act_spec, P("cp"), P("fsdp"), proj_spec, proj_spec, proj_spec, wout_spec), out_specs=(act_spec, act_spec, P("fsdp"), proj_spec, proj_spec, proj_spec, wout_spec), check_vma=False)
```

```python
import functools
import math

import jax
import jax.numpy as jnp
from jax import lax
from jax.experimental import pallas as pl
from jax.experimental.pallas import tpu as pltpu
from jax.sharding import PartitionSpec as P

WINDOW_LEN = 4096
ROPE_BASE = 10000.0
NORM_EPS = 1e-5
NEG_BIG = -1e30
LOG2E = math.log2(math.e)
BF16, F32 = jnp.bfloat16, jnp.float32
VMEM_LIMIT = 56 * 1024 * 1024
VMEM_ALL = 67_043_328
ATTN_TILE = 256


def dot(lhs, rhs, lhs_dim, rhs_dim):
    return lax.dot_general(lhs, rhs, (((lhs_dim,), (rhs_dim,)), ((), ())), preferred_element_type=F32)


def gather_ring(up, down, low, high, gate):
    one_low, back_high = up(low), down(high)
    one_high, back_low = up(high), down(low)
    one_low, back_high = gate((one_low, back_high))
    return {0: (low, high), 1: (one_low, one_high), 3: (back_low, back_high), 2: (up(one_low), down(back_high))}


def shift(axis, size, step):
    pairs = [(src, (src + step) % size) for src in range(size)]
    return lambda vals: lax.ppermute(vals, axis, pairs)


def swap_cores(vals):
    return lax.ppermute(vals, "fsdp", [(src, src ^ 1) for src in range(8)])


def rotate(vals, cosines, sines, sign):
    return vals * cosines + pltpu.roll(vals, vals.shape[1] // 2, 1) * (sines * sign)


def proj_kernel(rope_tiles, head_dim, x_ref, w_ref, cos_ref, sin_ref, o_ref):
    prod = jnp.dot(x_ref[...], w_ref[...], preferred_element_type=F32)

    def rotated():
        for head in range(prod.shape[1] // head_dim):
            cols = slice(head * head_dim, (head + 1) * head_dim)
            o_ref[:, cols] = rotate(prod[:, cols], cos_ref[...], sin_ref[...], 1.0).astype(BF16)

    if rope_tiles >= pl.num_programs(0):
        rotated()
    else:
        pl.when(pl.program_id(0) < rope_tiles)(rotated)

        @pl.when(pl.program_id(0) >= rope_tiles)
        def _():
            o_ref[...] = prod.astype(BF16)


def project(normed, weight, cosines, sines, rope_tiles):
    rows, depth = normed.shape
    cols, tile = weight.shape[1], 512
    head_dim = cosines.shape[1]
    whole = lambda shape: pl.BlockSpec(shape, lambda i: (0, 0))
    return pl.pallas_call(
        functools.partial(proj_kernel, rope_tiles, head_dim),
        grid=(cols // tile,),
        in_specs=[whole((rows, depth)), pl.BlockSpec((depth, tile), lambda i: (0, i)), whole((rows, head_dim)), whole((rows, head_dim))],
        out_specs=pl.BlockSpec((rows, tile), lambda i: (0, i)),
        out_shape=jax.ShapeDtypeStruct((rows, cols), BF16),
        compiler_params=pltpu.CompilerParams(vmem_limit_bytes=VMEM_LIMIT),
        cost_estimate=pl.CostEstimate(flops=2 * rows * depth * cols, bytes_accessed=2 * depth * (rows + cols), transcendentals=0),
        name="project",
    )(normed, weight, cosines, sines)


def block_mask(shape, key_dim, q_start, key_start):
    q_idx = q_start + lax.broadcasted_iota(jnp.int32, shape, 1 - key_dim)
    k_idx = key_start + lax.broadcasted_iota(jnp.int32, shape, key_dim)
    return (k_idx <= q_idx) & (k_idx > q_idx - WINDOW_LEN)


def needs_mask(block, length):
    return block == 0 or (block + 1) * length - 1 >= WINDOW_LEN


def attn_cost(products, length, width):
    return pl.CostEstimate(flops=products * length * length * width, bytes_accessed=25 * length * width, transcendentals=0)


def attn_fwd_kernel(tile, cp_ref, q_ref, *refs):
    k_refs, v_refs = refs[0:4], refs[4:8]
    o_ref, lse_ref = refs[8:]
    length, head_dim = q_ref.shape
    scale = head_dim**-0.5 * LOG2E

    def one_tile(blocks, step, carry):
        start = pl.multiple_of(step * tile, tile)
        q_blk = q_ref[pl.ds(start, tile), :]
        scores = []
        for block in range(blocks):
            part = dot(k_refs[block][...], q_blk, 1, 1)
            if needs_mask(block, length):
                part = jnp.where(block_mask(part.shape, 0, start, -block * length), part, NEG_BIG)
            scores.append(part)
        top = functools.reduce(jnp.maximum, [jnp.max(part, axis=0, keepdims=True) for part in scores]) * scale
        powers = [jnp.exp2(part * scale - top) for part in scores]
        total = sum(jnp.sum(part, axis=0, keepdims=True) for part in powers)
        inverse = 1.0 / total
        out = sum(dot(v_refs[block][...], (powers[block] * inverse).astype(BF16), 0, 0) for block in range(blocks))
        o_ref[pl.ds(start, tile), :] = out.T.astype(BF16)
        lse_ref[0, :, pl.ds(start, tile)] = jnp.broadcast_to(top + jnp.log2(total), (8, tile))
        return carry

    for rank in range(4):

        @pl.when(cp_ref[0] == rank)
        def _():
            lax.fori_loop(0, length // tile, functools.partial(one_tile, rank + 1), 0)


def attn_forward(rank, q_rot, kv_all, head_dim):
    length, width = q_rot.shape
    heads = width // head_dim
    kv_heads = kv_all.shape[2] // 2 // head_dim
    group = heads // kv_heads
    tile = ATTN_TILE
    q_spec = pl.BlockSpec((length, head_dim), lambda h, cp: (0, h))
    kv_spec = lambda o, first: pl.BlockSpec((None, length, head_dim), lambda h, cp: (lax.rem(cp[0] + 4 - o, 4), 0, first + h // group))
    return pl.pallas_call(
        functools.partial(attn_fwd_kernel, tile),
        grid_spec=pltpu.PrefetchScalarGridSpec(
            num_scalar_prefetch=1,
            grid=(heads,),
            in_specs=[q_spec] + [kv_spec(o, first) for first in (0, kv_heads) for o in range(4)],
            out_specs=[q_spec, pl.BlockSpec((1, 8, length), lambda h, cp: (h, 0, 0))],
        ),
        out_shape=[jax.ShapeDtypeStruct((length, width), BF16), jax.ShapeDtypeStruct((heads, 8, length), F32)],
        compiler_params=pltpu.CompilerParams(vmem_limit_bytes=VMEM_LIMIT),
        cost_estimate=attn_cost(16, length, width),
        name="attn_forward",
    )(rank, q_rot, *[kv_all] * 8)


def attn_bwd_kernel(tile, cp_ref, q_ref, do_ref, o_ref, lse_ref, cos_ref, sin_ref, *refs):
    k_refs, v_refs = refs[0:4], refs[4:8]
    dq_ref, dk_refs, dv_refs = refs[8], refs[9:13], refs[13:17]
    length, head_dim = q_ref.shape
    score_scale = head_dim**-0.5
    scale = score_scale * LOG2E

    @pl.when(pl.program_id(1) == 0)
    def _():
        for ref in (*dk_refs, *dv_refs):
            ref[...] = jnp.zeros_like(ref)

    def one_tile(blocks, step, carry):
        start = pl.multiple_of(step * tile, tile)
        rows = pl.ds(start, tile)
        q_blk, do_blk = q_ref[rows, :], do_ref[rows, :]
        row_dot = jnp.sum((do_blk.astype(F32) * o_ref[rows, :].astype(F32)).T, axis=0, keepdims=True)
        log_norm = lse_ref[0, 0:1, rows]
        d_query = jnp.zeros((tile, head_dim), F32)
        for block in range(blocks):
            k_blk, v_blk = k_refs[block][...], v_refs[block][...]
            probs = jnp.exp2(dot(k_blk, q_blk, 1, 1) * scale - log_norm)
            if needs_mask(block, length):
                probs = jnp.where(block_mask(probs.shape, 0, start, -block * length), probs, 0.0)
            d_scores = (probs * (dot(v_blk, do_blk, 1, 1) - row_dot) * score_scale).astype(BF16)
            dv_refs[block][...] += jnp.dot(probs.astype(BF16), do_blk, preferred_element_type=F32)
            dk_refs[block][...] += jnp.dot(d_scores, q_blk, preferred_element_type=F32)
            d_query += dot(d_scores, k_blk, 0, 0)
        dq_ref[rows, :] = rotate(d_query, cos_ref[rows, :], sin_ref[rows, :], -1.0).astype(BF16)
        return carry

    for rank in range(4):

        @pl.when(cp_ref[0] == rank)
        def _():
            lax.fori_loop(0, length // tile, functools.partial(one_tile, rank + 1), 0)


def attn_backward(rank, q_rot, d_attn, attn_out, log_norm, cosines, sines, kv_all):
    length, width = q_rot.shape
    head_dim = cosines.shape[1]
    heads, kv_heads = width // head_dim, kv_all.shape[2] // 2 // head_dim
    group = heads // kv_heads
    tile = ATTN_TILE
    q_spec = pl.BlockSpec((length, head_dim), lambda g, h, cp: (0, g * group + h))
    kv_spec = pl.BlockSpec((length, head_dim), lambda g, h, cp: (0, g))
    table = pl.BlockSpec((length, head_dim), lambda g, h, cp: (0, 0))
    kv_in = lambda o, first: pl.BlockSpec((None, length, head_dim), lambda g, h, cp: (lax.rem(cp[0] + 4 - o, 4), 0, first + g))
    kv_grad = jax.ShapeDtypeStruct((length, kv_heads * head_dim), F32)
    outs = pl.pallas_call(
        functools.partial(attn_bwd_kernel, tile),
        grid_spec=pltpu.PrefetchScalarGridSpec(
            num_scalar_prefetch=1,
            grid=(kv_heads, group),
            in_specs=[q_spec, q_spec, q_spec, pl.BlockSpec((1, 8, length), lambda g, h, cp: (g * group + h, 0, 0)), table, table] + [kv_in(o, first) for first in (0, kv_heads) for o in range(4)],
            out_specs=[q_spec] + [kv_spec] * 8,
        ),
        out_shape=[jax.ShapeDtypeStruct((length, width), BF16)] + [kv_grad] * 8,
        compiler_params=pltpu.CompilerParams(vmem_limit_bytes=VMEM_LIMIT),
        cost_estimate=attn_cost(40, length, width),
        name="attn_backward",
    )(rank, q_rot, d_attn, attn_out, log_norm, cosines, sines, *[kv_all] * 8)
    return outs[0], outs[1:5], outs[5:9]


def kv_grad_kernel(dk_ref, dv_ref, cos_ref, sin_ref, o_ref):
    head_dim, width = cos_ref.shape[1], dk_ref.shape[1]
    for head in range(width // head_dim):
        cols = slice(head * head_dim, (head + 1) * head_dim)
        o_ref[:, cols] = rotate(dk_ref[:, cols], cos_ref[...], sin_ref[...], -1.0).astype(BF16)
    o_ref[:, width:] = dv_ref[...].astype(BF16)


def kv_grad(d_keys, d_vals, cosines, sines):
    rows, width = d_keys.shape
    return pl.pallas_call(
        kv_grad_kernel,
        out_shape=jax.ShapeDtypeStruct((rows, 2 * width), BF16),
        compiler_params=pltpu.CompilerParams(vmem_limit_bytes=VMEM_LIMIT),
        name="kv_grad",
    )(d_keys, d_vals, cosines, sines)


MESH = pl.DeviceIdType.MESH


class Exchange:
    def __init__(self, collective_id):
        self.collective_id = collective_id
        self.entries, self.ins, self.in_specs, self.outs, self.out_specs, self.scratch = [], [], [], [], [], []
        self.sends = self.locals = 0

    def add(self, stages, axis, ins, outs, scratch, sends, locals_, space, out_space=pltpu.VMEM):
        self.entries.append((stages, axis, len(ins), len(outs), len(scratch), self.sends, self.locals))
        self.ins += ins
        spaces = space if isinstance(space, list) else [space] * len(ins)
        self.in_specs += [pl.BlockSpec(memory_space=kind) for kind in spaces]
        self.outs += outs
        self.out_specs += [pl.BlockSpec(memory_space=out_space)] * len(outs)
        self.scratch += scratch
        self.sends += sends
        self.locals += locals_

    def kernel(self, *refs):
        ins, refs = refs[: len(self.ins)], refs[len(self.ins) :]
        outs, refs = refs[: len(self.outs)], refs[len(self.outs) :]
        scratch, (send, recv, local) = refs[:-3], refs[-3:]
        where = {name: lax.axis_index(name) for name in ("tp", "cp", "fsdp")}
        quad = (4, (1, 3))
        steps = {"tp": quad, "cp": quad, "fsdp": (8, (2, 6))}
        wide = any(axis == "all" for _, axis, *_ in self.entries)
        steps_of = lambda axis: range(1, steps[axis][0]) if wide else steps[axis][1]
        axes = sorted({axis for _, axis, *_ in self.entries if axis not in ("all", "none")} | ({"tp", "cp", "fsdp"} if wide else set()))
        peers = [(axis, lax.rem(where[axis] + step, steps[axis][0])) for axis in axes for step in steps_of(axis)]
        barrier = pltpu.get_barrier_semaphore()
        for axis, peer in peers:
            pl.semaphore_signal(barrier, inc=1, device_id={axis: peer}, device_id_type=MESH)
        pl.semaphore_wait(barrier, len(peers))

        running = []
        for stages, axis, n_in, n_out, n_scratch, first_send, first_local in self.entries:

            def start(index, src, dst, axis, step, first_send=first_send):
                peer = lax.rem(where[axis] + step, steps[axis][0])
                sems = first_send + index
                copy = pltpu.make_async_remote_copy(src_ref=src, dst_ref=dst, send_sem=send.at[sems], recv_sem=recv.at[sems], device_id={axis: peer}, device_id_type=MESH)
                copy.start()
                return copy

            def load(index, src, dst, first_local=first_local):
                copy = pltpu.make_async_copy(src, dst, local.at[first_local + index])
                copy.start()
                return copy

            ring, place = start, where
            if axis not in ("all", "none"):
                size, (up, down) = steps[axis]
                ring = (functools.partial(lambda start, axis, step, i, s, d: start(i, s, d, axis, step), start, axis, up), functools.partial(lambda start, axis, step, i, s, d: start(i, s, d, axis, step), start, axis, down))
                place = where[axis] if size == 4 else where[axis] // 2
            running.append(stages(ins[:n_in], outs[:n_out], scratch[:n_scratch], ring, load, place))
            ins, outs, scratch = ins[n_in:], outs[n_out:], scratch[n_scratch:]
        left, closing = [], []
        while running:
            turns = [(stage, next(stage, stage)) for stage in running]
            left += [copy for _, copies in turns if isinstance(copies, list) for copy in copies]
            closing += [copies for stage, copies in turns if callable(copies)]
            running = [stage for stage, copies in turns if copies is not stage]
        for copy in left:
            copy.wait()
        for close in closing:
            close()

    def run(self):
        return pl.pallas_call(
            self.kernel,
            in_specs=self.in_specs,
            out_specs=self.out_specs,
            out_shape=self.outs,
            scratch_shapes=self.scratch + [pltpu.SemaphoreType.DMA((self.sends,)), pltpu.SemaphoreType.DMA((self.sends,)), pltpu.SemaphoreType.DMA((max(self.locals, 1),))],
            compiler_params=pltpu.CompilerParams(collective_id=self.collective_id, has_side_effects=True, vmem_limit_bytes=VMEM_ALL),
            cost_estimate=pl.CostEstimate(flops=40_000_000_000, bytes_accessed=40_000_000, transcendentals=0),
            name=f"exchange_{self.collective_id}",
        )(*self.ins)

    def ring_sum(self, axis, part):
        parts = [part(o, h) for o in range(4) for h in range(2)]
        half = jax.ShapeDtypeStruct(parts[0].shape, F32)
        self.add(given_ring_stages, axis, parts, [half] * 2, [pltpu.VMEM((8, *half.shape), F32), pltpu.VMEM((6, *half.shape), F32)], 6, 10, pl.ANY, pl.ANY)

    def weight_ring(self, features, d_lin):
        rows, cols = features.shape[1], d_lin.shape[1] // 2
        half = jax.ShapeDtypeStruct((rows, cols), F32)
        scratch = [pltpu.VMEM((8, rows, cols), F32), pltpu.VMEM((6, rows, cols), F32), pltpu.VMEM(features.shape, BF16), pltpu.VMEM(d_lin.shape, BF16)]
        self.add(weight_ring_stages, "fsdp", [features, d_lin], [half, half], scratch, 6, 10, pl.ANY, pl.ANY)

    def out_ring(self, attn_out, w_o, x_cols):
        rows, width = attn_out.shape
        cols = x_cols.shape[1]
        scratch = [pltpu.VMEM((8, rows // 2, cols), F32), pltpu.VMEM((6, rows // 2, cols), F32), pltpu.VMEM((cols, width), BF16), pltpu.VMEM((rows, cols), BF16)]
        out = jax.ShapeDtypeStruct((rows, 4 * cols), BF16)
        self.add(out_ring_stages, "tp", [attn_out, x_cols, w_o], [out], scratch, 12, 2, [pltpu.VMEM, pltpu.VMEM, pl.ANY])

    def normed_ring(self, dq_lin, dkv_lin, w_kv, wq_ring, wq_other):
        rows, width = dq_lin.shape[0] // 2, dq_lin.shape[1]
        cols = w_kv.shape[0] // 4
        half = jax.ShapeDtypeStruct((rows, cols), F32)
        scratch = [pltpu.VMEM((8, rows, cols), F32), pltpu.VMEM((6, rows, cols), F32), pltpu.VMEM((cols, width), BF16), pltpu.VMEM((cols, width), BF16)]
        self.add(normed_ring_stages, "tp", [dq_lin, dkv_lin, w_kv, wq_ring, wq_other], [half, half], scratch, 6, 10, [pltpu.VMEM] * 2 + [pl.ANY] * 3, pl.ANY)

    def project(self, normed, cosines, sines, wq_ring, wq_other):
        rows, depth = normed.shape
        cols = wq_ring.shape[2]
        scratch = [pltpu.VMEM((rows, depth), BF16), pltpu.VMEM((depth, cols), BF16)]
        self.add(project_stages, "none", [normed, cosines, sines, wq_ring, wq_other], [jax.ShapeDtypeStruct((rows, cols), BF16)], scratch, 0, 9, [pl.ANY, pltpu.VMEM, pltpu.VMEM, pl.ANY, pl.ANY])

    def all_sum(self, axis, low, high, head_dim, merged):
        heads = low.shape[2] // head_dim
        shape = lambda count: jax.ShapeDtypeStruct((4 * low.shape[1], count * heads, head_dim), F32)
        outs = [shape(2)] if merged else [shape(1)] * 2
        scratch = [pltpu.VMEM((6, *low.shape[1:]), F32), pltpu.VMEM((2, *low.shape[1:]), F32), pltpu.VMEM((2, *low.shape), F32)]
        self.add(all_sum_stages, axis, [low, high], outs, scratch, 12, 0, pltpu.VMEM)

    def gather(self, axis, block, by_columns, late=0, pause=1):
        shape = (block.shape[0], 4 * block.shape[1]) if by_columns else (4, *block.shape)
        self.add(functools.partial(gather_stages, by_columns, late, pause), axis, [block], [jax.ShapeDtypeStruct(shape, block.dtype)], [], 6, 1, pltpu.VMEM)

    def small_sum(self, vals):
        out = jax.ShapeDtypeStruct((4, *vals.shape), F32)
        self.add(small_sum_stages, "all", [vals], [out], [pltpu.VMEM((10, *vals.shape), F32), pltpu.VMEM(vals.shape, F32)], 13, 0, pltpu.VMEM)


def add_rows(dst, *terms):
    step = math.gcd(dst.shape[0], 64)

    def body(index, carry):
        rows = pl.ds(pl.multiple_of(index * step, step), step)
        dst[rows, :] = sum(term[rows, :] for term in terms)
        return carry

    lax.fori_loop(0, dst.shape[0] // step, body, 0)


def reduce_steps(term, into, land, ring, compute, pause=1):
    ways = list(zip(range(2), ring, (1, 3)))
    far, near, last = [], [], []
    for h, send, _ in ways:
        compute(2, h)
        far.append(send(h, term(2, h), land.at[h]))
    yield
    for h, send, o in ways:
        compute(o, 1 - h)
        near.append(send(2 + h, term(o, 1 - h), land.at[2 + h]))
        compute(o, h)
        yield
    for h, send, o in ways:
        far[h].wait()
        add_rows(into(o, h), term(o, h), land.at[h])
        last.append(send(4 + h, into(o, h), land.at[4 + h]))
    yield
    for h in range(2):
        compute(0, h)
    for _ in range(pause):
        yield
    for copy in near:
        copy.wait()
    yield
    for h in range(2):
        last[h].wait()
        add_rows(into(0, h), term(0, h), land.at[4 + h], land.at[3 - h])


def gather_steps(source, at, ring, place, base, pause):
    up, down = ring
    ways = list(zip(range(2), (up, down), (down, up), (3, 1)))
    first, more = [], []
    for h, send, _, _ in ways:
        first.append(send(base + h, source(h), at(place, h)))
    for h, _, send, _ in ways:
        more.append(send(base + 2 + h, source(h), at(place, h)))
    for _ in range(pause):
        yield
    for h, send, _, step in ways:
        from_next = at(lax.rem(place + step, 4), h)
        first[h].wait()
        more.append(send(base + 4 + h, from_next, from_next))
    yield more


def store_halves(parts, outs, load, base):
    yield [load(base + h, parts.at[h], outs[h]) for h in range(2)]


def given_ring_stages(ins, outs, scratch, ring, load, place):
    parts, land = scratch
    loads = {slot: load(slot, ins[slot], parts.at[slot]) for slot in (4, 5, 3, 2, 6, 7, 0, 1)}
    term = lambda o, h: parts.at[2 * o + h]
    yield from reduce_steps(term, term, land, ring, lambda o, h: loads[2 * o + h].wait(), 6)
    yield from store_halves(parts, outs, load, 8)


def weight_ring_stages(ins, outs, scratch, ring, load, place):
    parts, land, features, d_lin = scratch
    loads = [load(0, ins[0], features), load(1, ins[1], d_lin)]
    cols = parts.shape[2]
    yield
    for copy in loads:
        copy.wait()

    def compute(o, h):
        parts[2 * o + h] = jnp.dot(features[lax.rem(place + o, 4)], d_lin[:, h * cols : (h + 1) * cols], preferred_element_type=F32)

    term = lambda o, h: parts.at[2 * o + h]
    yield from reduce_steps(term, term, land, ring, compute, 6)
    yield from store_halves(parts, outs, load, 8)


def out_ring_stages(ins, outs, scratch, ring, load, place):
    (attn_out, x_cols, w_o), (parts, land, weights, block) = ins, scratch
    rows, cols = parts.shape[1], parts.shape[2]
    fetch = lambda o: load(0, w_o.at[pl.ds(pl.multiple_of(lax.rem(place + o, 4) * cols, cols), cols)], weights)
    following = {2: 1, 1: 3, 3: 0}
    pending, used = [fetch(2)], []
    yield

    def compute(o, h):
        while pending:
            pending.pop().wait()
        parts[2 * o + h] = dot(attn_out[h * rows : (h + 1) * rows, :], weights[...], 1, 1)
        if o in used and o in following:
            pending.append(fetch(following[o]))
        used.append(o)

    term = lambda o, h: parts.at[2 * o + h]
    yield from reduce_steps(term, term, land, ring, compute)
    for h in range(2):
        span = pl.ds(h * rows, rows)
        block[span, :] = (x_cols[span, :].astype(F32) + parts[h]).astype(BF16)
    shift_base = lambda i, src, dst: load(1 + i, src, dst)
    yield from gather_stages(True, 0, 1, (block,), outs, (), [functools.partial(rebase, send) for send in ring], shift_base, place)


def rebase(send, index, src, dst):
    return send(6 + index, src, dst)


def normed_ring_stages(ins, outs, scratch, ring, load, place):
    (dq, dkv, w_kv, wq_ring, wq_other), (parts, land, kv_weights, q_weights) = ins, scratch
    rows, cols = parts.shape[1], parts.shape[2]
    shard = cols // 2
    fsdp = lax.axis_index("fsdp")
    x_pos, core = fsdp // 2, lax.rem(fsdp, 2)
    loaded = [None]

    def fetch(o):
        chunk = lax.rem(place + o, 4)
        piece = lax.rem(x_pos + 4 - chunk, 4)
        copies = [
            load(0, w_kv.at[pl.ds(pl.multiple_of(chunk * cols, cols), cols)], kv_weights),
            load(1, wq_ring.at[piece], q_weights.at[pl.ds(pl.multiple_of(core * shard, shard), shard)]),
            load(2, wq_other.at[piece], q_weights.at[pl.ds(pl.multiple_of((1 - core) * shard, shard), shard)]),
        ]
        loaded[0] = (o, copies)

    fetch(2)
    yield
    following = {2: 1, 1: 3, 3: 0}
    used = {}

    def compute(o, h):
        if loaded[0][1] is not None:
            for copy in loaded[0][1]:
                copy.wait()
            loaded[0] = (o, None)
        span = slice(h * rows, (h + 1) * rows)
        parts[2 * o + h] = dot(dq[span, :], q_weights[...], 1, 1) + dot(dkv[span, :], kv_weights[...], 1, 1)
        used[o] = used.get(o, 0) + 1
        if used[o] == 2 and o in following:
            fetch(following[o])

    term = lambda o, h: parts.at[2 * o + h]
    yield from reduce_steps(term, term, land, ring, compute)
    yield from store_halves(parts, outs, load, 8)


def project_stages(ins, outs, scratch, ring, load, place):
    (normed, cosines, sines, wq_ring, wq_other), (out,), (x_buf, w_buf) = ins, outs, scratch
    shard, head_dim = wq_ring.shape[1], cosines.shape[1]
    x_pos, core = place["fsdp"] // 2, lax.rem(place["fsdp"], 2)
    loads = [load(0, normed, x_buf)]
    for o in range(4):
        for side, pieces in enumerate((wq_ring, wq_other)):
            owner = lax.rem(x_pos + 4 - o, 4) * 2 + (core if side == 0 else 1 - core)
            loads.append(load(1 + 2 * o + side, pieces.at[o], w_buf.at[pl.ds(pl.multiple_of(owner * shard, shard), shard)]))
    yield
    for copy in loads:
        copy.wait()
    tile = 256

    def body(step, carry):
        span = pl.ds(pl.multiple_of(step * tile, tile), tile)
        prod = jnp.dot(x_buf[...], w_buf[:, span], preferred_element_type=F32)
        heads = [rotate(prod[:, h * head_dim : (h + 1) * head_dim], cosines[...], sines[...], 1.0) for h in range(tile // head_dim)]
        out[:, span] = jnp.concatenate(heads, axis=1).astype(BF16)
        return carry

    lax.fori_loop(0, w_buf.shape[1] // tile, body, 0)


def all_sum_stages(ins, outs, scratch, ring, load, place):
    land, sums, whole = scratch
    term = lambda o, h: ins[h].at[lax.rem(place + o, 4)]
    at = lambda device, h: whole.at[h, device]
    into = lambda o, h: sums.at[h] if o else at(place, h)
    yield from reduce_steps(term, into, land, ring, lambda o, h: None)
    yield from gather_steps(lambda h: at(place, h), at, ring, place, 6, 1)

    def by_heads():
        rows, width = sums.shape[1:]
        head_dim = outs[0].shape[2]
        heads = width // head_dim
        for h in range(2):
            out, first = (outs[0], h * heads) if len(outs) == 1 else (outs[h], 0)
            for device in range(4):
                for head in range(heads):
                    out[pl.ds(device * rows, rows), first + head, :] = whole[h, device, :, head * head_dim : (head + 1) * head_dim]

    yield by_heads


def gather_stages(by_columns, late, pause, ins, outs, scratch, ring, load, place):
    (block,), (out,) = ins, outs
    rows, width = block.shape
    span = lambda h: pl.ds(h * (rows // 2), rows // 2)

    def at(device, rows):
        return out.at[rows, pl.ds(pl.multiple_of(device * width, width), width)] if by_columns else out.at[device, rows]

    for _ in range(late):
        yield
    mine = load(0, block, at(place, pl.ds(0, rows)))
    yield from gather_steps(lambda h: block.at[span(h)], lambda device, h: at(device, span(h)), ring, place, 0, pause)
    yield [mine]


def small_sum_stages(ins, outs, scratch, start, load, place):
    (vals,), (out,), (heard, told) = ins, outs, scratch
    over_y = [start(k - 1, vals, heard.at[k - 1], "cp", k) for k in range(1, 4)]
    yield
    for copy in over_y:
        copy.wait()
    told[...] = vals[...] + sum(heard[slot] for slot in range(3))
    over_x = [start(k + 2, told, heard.at[k + 2], "fsdp", k) for k in range(1, 8)]
    yield
    for copy in over_x:
        copy.wait()
    mine = place["tp"]
    out[mine] = told[...] + sum(heard[slot] for slot in range(3, 10))
    yield [start(k + 9, out.at[mine], out.at[mine], "tp", k) for k in range(1, 4)]


def solution(mesh):
    act_spec = P("fsdp", "cp", None)
    proj_spec = P("fsdp", "tp", None)
    wout_spec = P("tp", None, "fsdp")

    def device_step(hidden, cotangent, positions, gain, w_query, w_key, w_value, w_out):
        x_in, cot = hidden[0], cotangent[0]
        length, width = x_in.shape
        shard, q_heads, head_dim = w_query.shape
        kv_heads = w_key.shape[1]
        q_width, kv_width = q_heads * head_dim, kv_heads * head_dim
        quarter, cols = shard // 4, width // 4
        tp, cp, fsdp = lax.axis_index("tp"), lax.axis_index("cp"), lax.axis_index("fsdp")
        x_pos, core = fsdp // 2, fsdp % 2
        own_cols = lambda vals: lax.dynamic_slice_in_dim(vals, tp * cols, cols, -1)
        mat = lambda weight: weight.reshape(weight.shape[0], -1)
        tp_arr, cp_arr = jnp.reshape(tp, (1,)).astype(jnp.int32), jnp.reshape(cp, (1,)).astype(jnp.int32)
        x_up, x_down = shift("fsdp", 8, 2), shift("fsdp", 8, -2)

        def gather_weight(mat):
            mine = lax.dynamic_slice_in_dim(mat, cp * quarter, quarter)
            return lax.all_gather(mine, ("fsdp", "cp"), tiled=True)

        gains = jnp.stack([gain] + [shift("fsdp", 8, -2 * k)(gain) for k in range(1, 4)])
        others = swap_cores(gains)
        gains = jnp.stack([jnp.where(core == 0, gains, others), jnp.where(core == 0, others, gains)], axis=1)
        gain_full = lax.dynamic_slice_in_dim(jnp.concatenate([gains, gains]), 4 - x_pos, 4).reshape(width).astype(F32)

        w_kv = gather_weight(jnp.concatenate([mat(w_key), mat(w_value)], axis=1))
        w_o = lax.all_gather(w_out.reshape(q_width, shard).T, "fsdp", tiled=True)

        wq_mine = mat(w_query)
        wq_mine, gain_full = lax.optimization_barrier((wq_mine, gain_full))
        inv_freq = ROPE_BASE ** (-jnp.arange(0, head_dim, 2).astype(F32) / head_dim)
        angles = positions.astype(F32)[:, None] * inv_freq[None, :]
        cosines = jnp.concatenate([jnp.cos(angles)] * 2, axis=1)
        sines = jnp.concatenate([-jnp.sin(angles), jnp.sin(angles)], axis=1)

        x_f = x_in.astype(F32)
        inv_rms = lax.rsqrt(jnp.mean(x_f * x_f, axis=-1, keepdims=True) + NORM_EPS)
        normed = (x_f * inv_rms * gain_full).astype(BF16)

        features = normed.T.reshape(4, 2, shard, length)
        kept, given = (lax.dynamic_index_in_dim(features, side, 1, keepdims=False) for side in (core, 1 - core))
        cot_t = cot.T
        x_cols = own_cols(x_in)
        cot_cols = own_cols(cot)
        local = lambda arrays: lax.optimization_barrier((*arrays, normed, kept, given, cot_t, x_cols, cot_cols))
        wq_ring = gather_ring(x_up, x_down, wq_mine[: shard // 2], wq_mine[shard // 2 :], lambda landed: local(landed)[:2])
        wq_ring = jnp.stack([part for o in range(4) for part in wq_ring[o]]).reshape(4, shard, q_width)
        wq_other = swap_cores(wq_ring)
        w_kv, normed, kept, given, cot_t, x_cols, cot_cols = local((w_kv,))

        kv_rot = project(normed, w_kv, cosines, sines, kv_width // 512)
        features = jnp.concatenate([kept, swap_cores(given)], axis=2)
        front = Exchange(3)
        front.gather("cp", kv_rot, False)
        front.project(normed, cosines, sines, wq_ring, wq_other)
        kv_all, q_rot = front.run()
        d_attn = dot(cot, w_o, 1, 0).astype(BF16)
        attn_out, log_norm = attn_forward(cp_arr, q_rot, kv_all, head_dim)
        grad_wo = lax.psum_scatter(dot(cot_t, attn_out, 1, 0), ("fsdp", "cp"), tiled=True)

        dq_lin, dk_parts, dv_parts = attn_backward(cp_arr, q_rot, d_attn, attn_out, log_norm, cosines, sines, kv_all)

        both_cores = lambda d_lin: jnp.concatenate([d_lin, swap_cores(d_lin)])
        by_cp = lambda part: part.reshape(4, quarter, part.shape[1])
        first = Exchange(0)
        first.ring_sum("cp", lambda o, h: (dk_parts if h == 0 else dv_parts)[(4 - o) % 4])
        first.weight_ring(features, both_cores(dq_lin))
        first.out_ring(attn_out, w_o, x_cols)
        d_keys, d_vals, gq_low, gq_high, block_out = first.run()

        dkv_lin = kv_grad(d_keys, d_vals, cosines, sines)

        second = Exchange(1)
        second.all_sum("cp", by_cp(gq_low), by_cp(gq_high), head_dim, True)
        second.weight_ring(features, both_cores(dkv_lin))
        second.normed_ring(dq_lin, dkv_lin, w_kv, wq_ring, wq_other)
        second.gather("cp", grad_wo, False, 6, 2)
        grad_query, gk, gv, dn_low, dn_high, grad_wo = second.run()

        x_cols, cot_cols = x_cols.astype(F32), cot_cols.astype(F32)
        d_normed = jnp.concatenate([dn_low, dn_high])
        gain_cols = own_cols(gain_full)
        x_hat = x_cols * inv_rms
        grad_gain = jnp.sum(d_normed * x_hat, axis=0)
        scaled = d_normed * gain_cols
        row_dot = jnp.sum(scaled * x_hat, axis=-1)
        row_dot = row_dot + sum(shift("tp", 4, k)(row_dot) for k in range(1, 4))
        grad_cols = (cot_cols + inv_rms * (scaled - x_hat * (row_dot / width)[:, None])).astype(BF16)
        grad_gain = jnp.pad(grad_gain, (0, 2048 - cols)).reshape(16, 128)

        third = Exchange(2)
        third.small_sum(grad_gain)
        third.all_sum("cp", by_cp(gk), by_cp(gv), head_dim, False)
        third.gather("tp", grad_cols, True, 0, 4)
        gain_all, grad_key, grad_value, grad_hidden = third.run()
        grad_wout = grad_wo.reshape(shard, q_width).T.reshape(q_heads, head_dim, shard)
        gain_all = gain_all.reshape(4, 2048)[:, :cols].reshape(width)
        grad_gain = lax.dynamic_slice_in_dim(gain_all, fsdp * shard, shard, 0)
        return block_out[None], grad_hidden[None], grad_gain, grad_query, grad_key, grad_value, grad_wout

    return jax.shard_map(device_step, mesh=mesh, in_specs=(act_spec, act_spec, P("cp"), P("fsdp"), proj_spec, proj_spec, proj_spec, wout_spec), out_specs=(act_spec, act_spec, P("fsdp"), proj_spec, proj_spec, proj_spec, wout_spec), check_vma=False)
```
